32 devices in a mesh: gz: 2 (over x), row: 4 (over y, core), col: 4 (over z).
Axes of the slice: x: 2, y: 2, z: 4, core: 2. Of those that a mesh axis runs over, the one named last changes fastest.
Arguments:
- sections: bfloat16 [4, 2048, 2048], P('gz', 'row', 'col'), may hold values from -6 to 6
- priors: int32 [2, 4, 8, 8], P(None, 'gz', 'row', 'col'), may hold values from -64 to 64
- row_order: int32 [8], replicated, may hold values from 0 to 7, each once
Outputs:
- mesh_flows: float32 [8, 64], P('row')
The draws below stay inside these ranges and needn't reach their ends.
Inputs may be any that keep to these rules, and one draw needn't show every extreme that they name: A permutation of the patch rows: mesh row m holds patch row row_order[m].
All inputs are finite; a program needn't handle non-finite values.
Results may differ from the reference program's by a relative error of at most 0.0003.
Values may be sent and summed in bfloat16 or wider, within the bound.
No kernel may reach another device: no remote copies, remote signals or barrier semaphores. Data moves between devices by JAX's collectives and lax.ppermute only.
A program may use at most 64 MiB of HBM per device.

```python
import math
import jax
import jax.numpy as jnp
from jax import lax

PATCH = 512
STRIDE = 256
LAGS = 128
MAXOFF = 64
HALO = 256
SECTIONS = 4
HEIGHT = 2048
WIDTH = 2048
GRID_R = 8
GRID_C = 8


def shared_shifts(key):
    shift_key = jax.random.fold_in(key, 4242)
    reach = MAXOFF // 8
    starts = jax.random.randint(jax.random.fold_in(shift_key, 1), (2, SECTIONS), -reach, reach + 1)
    slopes = jax.random.randint(jax.random.fold_in(shift_key, 2), (2, SECTIONS), -reach, reach + 1)
    return (starts, slopes)


def moved_by(starts, slopes, coords, extent):
    return starts[:, None] + slopes[:, None] * coords[None, :] // extent


def draw_sections(key, part):
    starts, slopes = shared_shifts(key)
    rows_all = jnp.arange(HEIGHT, dtype=jnp.int32)
    cols_all = jnp.arange(WIDTH, dtype=jnp.int32)
    row_shift = moved_by(starts[0], slopes[0], rows_all, HEIGHT)
    col_shift = moved_by(starts[1], slopes[1], cols_all, WIDTH)
    margin = MAXOFF
    texture_key = jax.random.fold_in(key, 11)
    noise_key = jax.random.fold_in(key, 12)
    texture = jax.random.normal(texture_key, (HEIGHT + 2 * margin, WIDTH + 2 * margin), jnp.float32)
    noise = jax.random.normal(noise_key, (SECTIONS, HEIGHT, WIDTH), jnp.float32)
    signal_weight = 0.9
    noise_weight = 0.45
    level = 1.0
    row_index = rows_all[None, :] - row_shift + margin
    col_index = cols_all[None, :] - col_shift + margin

    def one_section(row_pick, col_pick):
        return jnp.take(jnp.take(texture, row_pick, axis=0), col_pick, axis=1)
    moved = jax.vmap(one_section)(row_index, col_index)
    result = level * (signal_weight * moved + noise_weight * noise)
    return jnp.clip(result, -6.0, 6.0).astype(jnp.bfloat16)


def draw_priors(key, part):
    starts, slopes = shared_shifts(key)
    center_gap = PATCH // 2 - HALO // 2
    row_centers = jnp.clip(jnp.arange(GRID_R, dtype=jnp.int32) * STRIDE + center_gap, 0, HEIGHT - 1)
    col_centers = jnp.clip(jnp.arange(GRID_C, dtype=jnp.int32) * STRIDE + center_gap, 0, WIDTH - 1)
    row_shift = moved_by(starts[0], slopes[0], row_centers, HEIGHT)
    col_shift = moved_by(starts[1], slopes[1], col_centers, WIDTH)
    row_lag = jnp.roll(row_shift, -1, axis=0) - row_shift
    col_lag = jnp.roll(col_shift, -1, axis=0) - col_shift
    slack = MAXOFF // 2
    jitter = jax.random.randint(jax.random.fold_in(key, 13), (2, SECTIONS, GRID_R, GRID_C), -slack, slack + 1)
    row_prior = row_lag[:, :, None] + jitter[0]
    col_prior = col_lag[:, None, :] + jitter[1]
    result = jnp.clip(jnp.stack([row_prior, col_prior], axis=0), -MAXOFF, MAXOFF)
    result = result.at[0, 0, 0, 0].set(MAXOFF)
    result = result.at[0, SECTIONS - 1, 0, 0].set(-MAXOFF)
    result = result.at[1, 0, 0, 0].set(-MAXOFF)
    result = result.at[1, SECTIONS - 1, 0, 0].set(MAXOFF)
    return result.astype(jnp.int32)


def setup_inputs(seed: int = 0) -> dict:
    splits = jax.random.split(jax.random.key(seed), 4)
    sections = draw_sections(jax.random.fold_in(splits[3], 71), 0)
    priors = draw_priors(jax.random.fold_in(splits[3], 71), 0)
    row_order = jax.random.permutation(splits[2], GRID_R).astype(jnp.int32)
    return dict(sections=sections, priors=priors, row_order=row_order)


def dft_tables(length):
    frequencies = jnp.arange(length, dtype=jnp.int32)
    angles = jnp.mod(frequencies[:, None] * frequencies[None, :], length).astype(jnp.float32) * (2.0 * math.pi / length)
    cosine = jnp.cos(angles)
    sine_part = jnp.sin(angles)
    minus_table = jnp.concatenate([cosine, -sine_part], axis=1).astype(jnp.bfloat16)
    plus_table = jnp.concatenate([cosine, sine_part], axis=1).astype(jnp.bfloat16)
    return minus_table, plus_table


def spectra_of(patches, minus_table, plus_table):
    length = patches.shape[-1]
    row_pass = jnp.einsum('nxy,yk->nxk', patches.astype(jnp.float32), minus_table.astype(jnp.float32)).astype(jnp.bfloat16)
    real_rows = row_pass[:, :, :length]
    imag_rows = row_pass[:, :, length:]
    upper_stack = jnp.concatenate([real_rows, imag_rows], axis=1).astype(jnp.float32)
    lower_stack = jnp.concatenate([imag_rows, real_rows], axis=1).astype(jnp.float32)
    spec_real = jnp.einsum('kx,nxm->nkm', plus_table.astype(jnp.float32), upper_stack) / length
    spec_imag = jnp.einsum('kx,nxm->nkm', minus_table.astype(jnp.float32), lower_stack) / length
    return jnp.stack([spec_real, spec_imag], axis=1).astype(jnp.bfloat16)


def lag_angles(offsets, length):
    frequencies = jnp.arange(length, dtype=jnp.int32)
    shifts = offsets[:, None] + jnp.arange(LAGS, dtype=jnp.int32)[None, :] - LAGS // 2
    angles = jnp.mod(shifts[:, :, None] * frequencies[None, None, :], length).astype(jnp.float32) * (2.0 * math.pi / length)
    return jnp.cos(angles), jnp.sin(angles)


def flows_of(first_spec, second_spec, offsets):
    length = first_spec.shape[-1]
    first_real = first_spec[:, 0].astype(jnp.float32)
    first_imag = first_spec[:, 1].astype(jnp.float32)
    second_real = second_spec[:, 0].astype(jnp.float32)
    second_imag = second_spec[:, 1].astype(jnp.float32)
    prod_real = (first_real * second_real + first_imag * second_imag).astype(jnp.bfloat16)
    prod_imag = (first_real * second_imag - first_imag * second_real).astype(jnp.bfloat16)
    row_cosine, row_sine = lag_angles(offsets[0], length)
    column_cosine, column_sine = lag_angles(offsets[1], length)
    products = jnp.concatenate([prod_real, prod_imag], axis=2).astype(jnp.float32)
    column_real = jnp.concatenate([column_cosine, -column_sine], axis=2).astype(jnp.bfloat16).astype(jnp.float32)
    column_imag = jnp.concatenate([column_sine, column_cosine], axis=2).astype(jnp.bfloat16).astype(jnp.float32)
    half_real = jnp.einsum('nkl,nul->nku', products, column_real).astype(jnp.bfloat16)
    half_imag = jnp.einsum('nkl,nul->nku', products, column_imag).astype(jnp.bfloat16)
    row_table = jnp.concatenate([row_cosine, -row_sine], axis=2).astype(jnp.bfloat16).astype(jnp.float32)
    stacked = jnp.concatenate([half_real, half_imag], axis=1).astype(jnp.float32)
    surface = jnp.einsum('ntk,nku->ntu', row_table, stacked) / length
    weights = surface * surface
    displacement = (jnp.arange(LAGS, dtype=jnp.int32) - LAGS // 2).astype(jnp.float32)
    weight_sum = 1.0 + jnp.sum(weights, axis=(1, 2))
    row_shift = jnp.sum(weights * displacement[None, :, None], axis=(1, 2)) / weight_sum
    column_shift = jnp.sum(weights * displacement[None, None, :], axis=(1, 2)) / weight_sum
    return jnp.stack([offsets[0].astype(jnp.float32) + row_shift, offsets[1].astype(jnp.float32) + column_shift], axis=0)


def reference(sections, priors, row_order):
    minus_table, plus_table = dft_tables(PATCH)
    margin = HALO // 2
    padded = jnp.pad(sections, ((0, 0), (margin, HALO - margin), (margin, HALO - margin)))
    place_count = GRID_R * GRID_C
    offsets_all = jnp.transpose(priors, (2, 3, 0, 1)).reshape(place_count, 2, SECTIONS)
    positions = jnp.arange(place_count, dtype=jnp.int32)

    def one_place(inputs):
        position, offsets = inputs
        top_edge = (position // GRID_C) * STRIDE
        left_edge = (position % GRID_C) * STRIDE
        window = lax.dynamic_slice(padded, (jnp.int32(0), top_edge.astype(jnp.int32), left_edge.astype(jnp.int32)), (SECTIONS, PATCH, PATCH))
        spectra = spectra_of(window, minus_table, plus_table)
        following = jnp.concatenate([spectra[1:], spectra[:1]], axis=0)
        return flows_of(spectra, following, offsets)

    all_flows = lax.map(one_place, (positions, offsets_all))
    flow_table = jnp.transpose(all_flows.reshape(GRID_R, GRID_C, 2, SECTIONS), (2, 3, 0, 1))
    picked = flow_table[:, :, row_order, :]
    return jnp.transpose(picked, (2, 0, 1, 3)).reshape(GRID_R, 2 * SECTIONS * GRID_C)
```

```python
import functools
import math

import jax
import jax.numpy as jnp
import numpy as np
from jax import lax
from jax.experimental import pallas as pl
from jax.experimental.pallas import tpu as pltpu
from jax.sharding import PartitionSpec as P

PATCH = 512
STRIDE = 256
LAGS = 128
MAXOFF = 64
HALO = 256
HALF = PATCH // 2
MARGIN = HALO // 2
AXES = ("gz", "row", "col")


def frequency_tables():
    frequencies = np.arange(HALF)[:, None]
    places = np.arange(PATCH)[None, :]
    step = 2.0 * math.pi / PATCH
    cosine = np.cos(np.mod(frequencies * places, PATCH) * step)
    sine_part = np.sin(np.mod(frequencies * places, PATCH) * step)
    sine_part[0] = np.cos(np.mod(HALF * places[0], PATCH) * step)
    table = np.concatenate([cosine, sine_part], axis=0)
    lags = np.arange(-MAXOFF - LAGS // 2, MAXOFF + LAGS // 2) % PATCH
    return table.astype(np.float32), table.T[lags].astype(np.float32)


def neighbours(value, axis, dim, width):
    devices, length = (lax.axis_size(axis), value.shape[dim])
    up = [(i, i + 1) for i in range(devices - 1)]
    down = [(j, i) for i, j in up]
    last = lax.slice_in_dim(value, length - width, length, axis=dim)
    first = lax.slice_in_dim(value, 0, width, axis=dim)
    return lax.ppermute(last, axis, up), lax.ppermute(first, axis, down)


def split_parts(spec_ref, out_ref):
    for rows, cols in ((slice(0, 16), slice(0, HALF)), (slice(16, HALF), slice(0, 128)), (slice(16, HALF), slice(128, HALF))):
        low_r = slice(rows.start + HALF, rows.stop + HALF)
        low_c = slice(cols.start + HALF, cols.stop + HALF)
        cc = spec_ref[rows, cols]
        cs = spec_ref[rows, low_c]
        sc = spec_ref[low_r, cols]
        ss = spec_ref[low_r, low_c]
        a, b, c, d = cc - ss, sc + cs, cc + ss, sc - cs
        if cols.start == 0:
            edge = lax.broadcasted_iota(jnp.int32, cc.shape, 1) == 0
            a, b, c, d = jnp.where(edge, cc, a), jnp.where(edge, sc, b), jnp.where(edge, cs, c), jnp.where(edge, ss, d)
        if rows.start == 0:
            edge = lax.broadcasted_iota(jnp.int32, cc.shape, 0) == 0
            a, b, c, d = jnp.where(edge, cc, a), jnp.where(edge, cs, b), jnp.where(edge, sc, c), jnp.where(edge, ss, d)
        out_ref[0, rows, cols] = a.astype(out_ref.dtype)
        out_ref[1, rows, cols] = b.astype(out_ref.dtype)
        out_ref[2, rows, cols] = c.astype(out_ref.dtype)
        out_ref[3, rows, cols] = d.astype(out_ref.dtype)


def cross_parts(first_ref, second_ref, out_ref):
    for rows, cols in ((slice(0, 16), slice(0, HALF)), (slice(16, HALF), slice(0, 128)), (slice(16, HALF), slice(128, HALF))):
        low_r = slice(rows.start + HALF, rows.stop + HALF)
        low_c = slice(cols.start + HALF, cols.stop + HALF)
        a, b, c, d = (first_ref[n, rows, cols].astype(jnp.float32) for n in range(4))
        e, f, g, h = (second_ref[n, rows, cols].astype(jnp.float32) for n in range(4))
        p, u = a * e + b * f, a * f - b * e
        q, v = c * g + d * h, c * h - d * g
        cc, cs, sc, ss = p + q, u - v, u + v, q - p
        if cols.start == 0:
            edge = lax.broadcasted_iota(jnp.int32, cc.shape, 1) == 0
            cc, cs, sc, ss = jnp.where(edge, p, cc), jnp.where(edge, q, cs), jnp.where(edge, u, sc), jnp.where(edge, v, ss)
        if rows.start == 0:
            row = lax.broadcasted_iota(jnp.int32, cc.shape, 0) == 0
            cc, cs, sc, ss = jnp.where(row, p, cc), jnp.where(row, u, cs), jnp.where(row, q, sc), jnp.where(row, v, ss)
            corner = jnp.logical_and(row, lax.broadcasted_iota(jnp.int32, cc.shape, 1) == 0)
            cc, cs = jnp.where(corner, 0.5 * (a * e), cc), jnp.where(corner, 0.5 * (b * f), cs)
            sc, ss = jnp.where(corner, 0.5 * (c * g), sc), jnp.where(corner, 0.5 * (d * h), ss)
        out_ref[rows, cols] = cc.astype(jnp.bfloat16)
        out_ref[rows, low_c] = cs.astype(jnp.bfloat16)
        out_ref[low_r, cols] = sc.astype(jnp.bfloat16)
        out_ref[low_r, low_c] = ss.astype(jnp.bfloat16)


def lag_rows(lag_ref, offset):
    pieces = [lag_ref[n, pl.ds(offset + MAXOFF, LAGS), :] for n in range(lag_ref.shape[0])]
    return jnp.concatenate(pieces, axis=1).astype(jnp.bfloat16)


def match_kernel(
    meta_ref, table_ref, turned_ref, lag_ref, own_ref, arrived_ref, left_ref, right_ref, above_ref, below_ref,
    out_ref, ext_ref, rows_ref, spec_ref, part_ref, cross_ref, *, sizes,
):
    size_gz, size_row, size_col, sec_count, per_side = sizes
    side = per_side * STRIDE
    top, wide = side + MARGIN, side + HALO
    place_count = per_side * per_side
    for s in range(sec_count + 1):
        center = own_ref[s] if s < sec_count else arrived_ref[0]
        ext_ref[0:MARGIN, :] = above_ref[s]
        ext_ref[MARGIN:top, 0:MARGIN] = left_ref[s]
        ext_ref[MARGIN:top, MARGIN:top] = center
        ext_ref[MARGIN:top, top:wide] = right_ref[s]
        ext_ref[top:wide, :] = below_ref[s]
        for pj in range(per_side):
            rows_ref[...] = jnp.dot(
                ext_ref[:, pj * STRIDE : pj * STRIDE + PATCH], turned_ref[...], preferred_element_type=jnp.float32
            ).astype(jnp.bfloat16)
            for pi in range(per_side):
                spec_ref[...] = jnp.dot(
                    table_ref[...], rows_ref[pi * STRIDE : pi * STRIDE + PATCH, :], preferred_element_type=jnp.float32
                )
                split_parts(spec_ref, part_ref.at[s, pi * per_side + pj])

    lanes_each = 2 * size_gz * sec_count * size_col * per_side
    row_count = size_row * per_side
    rows_each = row_count // size_row
    shape = (size_row, rows_each * lanes_each)
    holder = lax.broadcasted_iota(jnp.int32, shape, 0)
    lane = lax.broadcasted_iota(jnp.int32, shape, 1)
    slot = jnp.zeros(shape, jnp.int32)
    head = 3 + 2 * sec_count * place_count
    for m in range(row_count):
        here = jnp.logical_and(holder == m // rows_each, lane // lanes_each == m % rows_each)
        slot = jnp.where(here, meta_ref[head + m], slot)
    lane = lane % lanes_each
    my_gz, my_row, my_col = meta_ref[0], meta_ref[1], meta_ref[2]
    total_out = jnp.zeros(shape, jnp.float32)
    scale = 2.0 / float(PATCH) ** 3
    down = (lax.broadcasted_iota(jnp.int32, (LAGS, LAGS), 0) - LAGS // 2).astype(jnp.float32)
    across = (lax.broadcasted_iota(jnp.int32, (LAGS, LAGS), 1) - LAGS // 2).astype(jnp.float32)
    for s in range(sec_count):
        for n in range(place_count):
            pi, pj = n // per_side, n % per_side
            cross_parts(part_ref.at[s, n], part_ref.at[s + 1, n], cross_ref)
            p = meta_ref[3 + s * place_count + n]
            q = meta_ref[3 + (sec_count + s) * place_count + n]
            row_lags = lag_rows(lag_ref, p)
            col_lags = lag_rows(lag_ref, q)
            half = lax.dot_general(
                cross_ref[...], col_lags, (((1,), (1,)), ((), ())), preferred_element_type=jnp.float32
            ).astype(jnp.bfloat16)
            surface = jnp.dot(row_lags, half, preferred_element_type=jnp.float32) * scale
            weights = surface * surface
            total = 1.0 + jnp.sum(weights, keepdims=True)
            shift_r = jnp.sum(weights * down, keepdims=True) / total
            shift_c = jnp.sum(weights * across, keepdims=True) / total
            mine = slot == my_row * per_side + pi
            place = (my_gz * sec_count + s) * (size_col * per_side) + my_col * per_side + pj
            half_lanes = lanes_each // 2
            total_out += jnp.where(jnp.logical_and(mine, lane == place), p.astype(jnp.float32) + shift_r, 0.0)
            total_out += jnp.where(jnp.logical_and(mine, lane == place + half_lanes), q.astype(jnp.float32) + shift_c, 0.0)
    for g in range(size_gz):
        for r in range(size_row):
            out_ref[(g * size_row + r) * size_col : (g * size_row + r + 1) * size_col, :] = jnp.broadcast_to(
                total_out[r : r + 1, :], (size_col, shape[1])
            )


def body(sections, priors, row_order):
    sec_count, side = sections.shape[:2]
    per_side = side // STRIDE
    size_gz, size_row, size_col = (lax.axis_size(a) for a in AXES)
    table, lag_table = frequency_tables()
    table = jnp.asarray(table).astype(jnp.bfloat16)
    turned = jnp.asarray(frequency_tables()[0].T).astype(jnp.bfloat16)
    lag_table = jnp.asarray(np.stack(np.split(lag_table, PATCH // 128, axis=1))).astype(jnp.bfloat16).astype(jnp.float32)
    arrived = lax.ppermute(sections[:1], "gz", [(i, (i - 1) % size_gz) for i in range(size_gz)])
    all_sections = jnp.concatenate([sections, arrived], axis=0)
    left, right = neighbours(all_sections, "col", 2, MARGIN)
    def edge_rows(a, b):
        return jnp.concatenate([left[:, a:b], all_sections[:, a:b], right[:, a:b]], axis=2)
    up = [(i, i + 1) for i in range(size_row - 1)]
    above = lax.ppermute(edge_rows(side - MARGIN, side), "row", up)
    below = lax.ppermute(edge_rows(0, MARGIN), "row", [(j, i) for i, j in up])
    meta = jnp.concatenate(
        [jnp.stack([lax.axis_index(a) for a in AXES]).astype(jnp.int32), priors.reshape(-1), row_order]
    )
    lanes = (row_order.shape[0] // size_row) * 2 * size_gz * sec_count * size_col * per_side
    devices = size_gz * size_row * size_col
    wide = side + HALO
    sizes = (size_gz, size_row, size_col, sec_count, per_side)
    vmem = pl.BlockSpec(memory_space=pltpu.VMEM)
    sent = pl.pallas_call(
        functools.partial(match_kernel, sizes=sizes),
        out_shape=jax.ShapeDtypeStruct((devices, lanes), jnp.float32),
        in_specs=[pl.BlockSpec(memory_space=pltpu.SMEM)] + [vmem] * 9,
        out_specs=vmem,
        scratch_shapes=[
            pltpu.VMEM((wide, wide), jnp.bfloat16),
            pltpu.VMEM((wide, PATCH), jnp.bfloat16),
            pltpu.VMEM((PATCH, PATCH), jnp.float32),
            pltpu.VMEM((sec_count + 1, per_side * per_side, 4, HALF, HALF), jnp.float32),
            pltpu.VMEM((PATCH, PATCH), jnp.bfloat16),
        ],
        name="match",
    )(meta, table, turned, lag_table, sections, arrived, left, right, above, below)
    received = lax.all_to_all(sent, AXES, 0, 0, tiled=True)
    return jnp.sum(received, axis=0).reshape(row_order.shape[0] // size_row, -1)


def solution(mesh):
    placed = (P("gz", "row", "col"), P(None, "gz", "row", "col"), P())
    return jax.shard_map(body, mesh=mesh, in_specs=placed, out_specs=P("row", None), check_vma=False)
```

```python
import functools
import math

import jax
import jax.numpy as jnp
import numpy as np
from jax import lax
from jax.experimental import pallas as pl
from jax.experimental.pallas import tpu as pltpu
from jax.sharding import PartitionSpec as P


PATCH = 512
STRIDE = 256
LAGS = 128
MAXOFF = 64
HALO = 256
HALF = PATCH // 2
MARGIN = HALO // 2
AXES = ("gz", "row", "col")
VMEM_LIMIT = 16 * 1024 * 1024
GLUE_FLOPS = 4 * 10**9


def frequency_tables():
    frequencies = np.arange(HALF)[:, None]
    places = np.arange(PATCH)[None, :]
    step = 2.0 * math.pi / PATCH
    cosine = np.cos(np.mod(frequencies * places, PATCH) * step)
    sine_part = np.sin(np.mod(frequencies * places, PATCH) * step)
    sine_part[0] = np.cos(np.mod(HALF * places[0], PATCH) * step)
    table = np.concatenate([cosine, sine_part], axis=0)
    lags = np.arange(-MAXOFF - LAGS // 2, MAXOFF + LAGS // 2) % PATCH
    return table.astype(np.float32), table.T[lags].astype(np.float32)


def split_parts(spec_ref, out_ref):
    for rows, cols in ((slice(0, 16), slice(0, HALF)), (slice(16, HALF), slice(0, 128)), (slice(16, HALF), slice(128, HALF))):
        low_r = slice(rows.start + HALF, rows.stop + HALF)
        low_c = slice(cols.start + HALF, cols.stop + HALF)
        cc = spec_ref[rows, cols]
        cs = spec_ref[rows, low_c]
        sc = spec_ref[low_r, cols]
        ss = spec_ref[low_r, low_c]
        a, b, c, d = cc - ss, sc + cs, cc + ss, sc - cs
        if cols.start == 0:
            edge = lax.broadcasted_iota(jnp.int32, cc.shape, 1) == 0
            a, b, c, d = jnp.where(edge, cc, a), jnp.where(edge, sc, b), jnp.where(edge, cs, c), jnp.where(edge, ss, d)
        if rows.start == 0:
            edge = lax.broadcasted_iota(jnp.int32, cc.shape, 0) == 0
            a, b, c, d = jnp.where(edge, cc, a), jnp.where(edge, cs, b), jnp.where(edge, sc, c), jnp.where(edge, ss, d)
        out_ref[0, rows, cols] = a.astype(out_ref.dtype)
        out_ref[1, rows, cols] = b.astype(out_ref.dtype)
        out_ref[2, rows, cols] = c.astype(out_ref.dtype)
        out_ref[3, rows, cols] = d.astype(out_ref.dtype)


def cross_parts(first_ref, second_ref, out_ref):
    for rows, cols in ((slice(0, 16), slice(0, HALF)), (slice(16, HALF), slice(0, 128)), (slice(16, HALF), slice(128, HALF))):
        low_r = slice(rows.start + HALF, rows.stop + HALF)
        low_c = slice(cols.start + HALF, cols.stop + HALF)
        a, b, c, d = (first_ref[n, rows, cols].astype(jnp.float32) for n in range(4))
        e, f, g, h = (second_ref[n, rows, cols].astype(jnp.float32) for n in range(4))
        p, u = a * e + b * f, a * f - b * e
        q, v = c * g + d * h, c * h - d * g
        cc, cs, sc, ss = p + q, u - v, u + v, q - p
        if cols.start == 0:
            edge = lax.broadcasted_iota(jnp.int32, cc.shape, 1) == 0
            cc, cs, sc, ss = jnp.where(edge, p, cc), jnp.where(edge, q, cs), jnp.where(edge, u, sc), jnp.where(edge, v, ss)
        if rows.start == 0:
            row = lax.broadcasted_iota(jnp.int32, cc.shape, 0) == 0
            cc, cs, sc, ss = jnp.where(row, p, cc), jnp.where(row, u, cs), jnp.where(row, q, sc), jnp.where(row, v, ss)
            corner = jnp.logical_and(row, lax.broadcasted_iota(jnp.int32, cc.shape, 1) == 0)
            cc, cs = jnp.where(corner, 0.5 * (a * e), cc), jnp.where(corner, 0.5 * (b * f), cs)
            sc, ss = jnp.where(corner, 0.5 * (c * g), sc), jnp.where(corner, 0.5 * (d * h), ss)
        out_ref[rows, cols] = cc.astype(jnp.bfloat16)
        out_ref[rows, low_c] = cs.astype(jnp.bfloat16)
        out_ref[low_r, cols] = sc.astype(jnp.bfloat16)
        out_ref[low_r, low_c] = ss.astype(jnp.bfloat16)


def lag_rows(lag_ref, offset):
    pieces = [lag_ref[n, pl.ds(offset + MAXOFF, LAGS), :] for n in range(lag_ref.shape[0])]
    return jnp.concatenate(pieces, axis=1).astype(jnp.bfloat16)


def fill_parts(table_ref, turned_ref, meta_ref, pieces, s, out_ref, ext_ref, rows_ref, spec_ref):
    center_refs, col_refs, row_refs = pieces
    top = ext_ref.shape[0] - MARGIN
    row_even, col_even = meta_ref[1] % 2 == 0, meta_ref[2] % 2 == 0
    inner, outer = row_refs[0][s], row_refs[1][s]
    ext_ref[0:MARGIN, :] = lax.select(row_even, outer, inner)
    ext_ref[top:, :] = lax.select(row_even, inner, outer)
    inner, outer = col_refs[0][s], col_refs[1][s]
    ext_ref[MARGIN:top, 0:MARGIN] = lax.select(col_even, outer, inner)
    ext_ref[MARGIN:top, top:] = lax.select(col_even, inner, outer)
    center_rows(ext_ref.at[MARGIN:top, MARGIN:top], col_even, center_refs, s, slice(0, top - MARGIN))
    per_side = (top - MARGIN) // STRIDE
    for pj in range(per_side):
        rows_ref[...] = jnp.dot(
            ext_ref[:, pj * STRIDE : pj * STRIDE + PATCH], turned_ref[...], preferred_element_type=jnp.float32
        ).astype(jnp.bfloat16)
        for pi in range(per_side):
            spec_ref[...] = jnp.dot(
                table_ref[...], rows_ref[pi * STRIDE : pi * STRIDE + PATCH, :], preferred_element_type=jnp.float32
            )
            split_parts(spec_ref, out_ref.at[pi * per_side + pj])


def center_rows(out_ref, col_even, center_refs, s, rows):
    if len(center_refs) == 1:
        out_ref[...] = center_refs[0][s, rows]
        return
    middle_ref, inner_ref, outer_ref = center_refs
    side = out_ref.shape[1]
    inner, outer = inner_ref[s, rows], outer_ref[s, rows]
    out_ref[:, 0:MARGIN] = lax.select(col_even, outer, inner)
    out_ref[:, MARGIN : side - MARGIN] = middle_ref[s, rows]
    out_ref[:, side - MARGIN :] = lax.select(col_even, inner, outer)


def cut_kernel(meta_ref, far_ref, inner_ref, outer_ref, first_inner_ref, first_outer_ref, middle_ref, own_ref):
    own_ref[...] = far_ref[...]
    side = own_ref.shape[2]
    col_even = meta_ref[2] % 2 == 0
    for s in range(own_ref.shape[0]):
        low, high = own_ref[s, :, 0:MARGIN], own_ref[s, :, side - MARGIN :]
        inner_ref[s] = lax.select(col_even, high, low)
        outer_ref[s] = lax.select(col_even, low, high)
    low, high = own_ref[0, :, 0:MARGIN], own_ref[0, :, side - MARGIN :]
    first_inner_ref[0] = lax.select(col_even, high, low)
    first_outer_ref[0] = lax.select(col_even, low, high)
    middle_ref[0] = own_ref[0, :, MARGIN : side - MARGIN]


def edge_kernel(meta_ref, *refs):
    *center_refs, col_inner_ref, col_outer_ref, inner_ref, outer_ref = refs
    side = col_inner_ref.shape[1]
    row_even, col_even = meta_ref[1] % 2 == 0, meta_ref[2] % 2 == 0
    low, high = slice(0, MARGIN), slice(side - MARGIN, side)
    for s in range(inner_ref.shape[0]):
        for ref, even_rows, odd_rows in ((inner_ref, high, low), (outer_ref, low, high)):
            def pick(source, start, stop):
                return lax.select(row_even, source[s, even_rows, start:stop], source[s, odd_rows, start:stop])

            inner, outer = pick(col_inner_ref, 0, MARGIN), pick(col_outer_ref, 0, MARGIN)
            ref[s, :, 0:MARGIN] = lax.select(col_even, outer, inner)
            ref[s, :, side + MARGIN :] = lax.select(col_even, inner, outer)
            if len(center_refs) == 1:
                ref[s, :, MARGIN : side + MARGIN] = pick(center_refs[0], 0, side)
            else:
                middle_ref, first_inner_ref, first_outer_ref = center_refs
                inner, outer = pick(first_inner_ref, 0, MARGIN), pick(first_outer_ref, 0, MARGIN)
                ref[s, :, MARGIN : 2 * MARGIN] = lax.select(col_even, outer, inner)
                ref[s, :, 2 * MARGIN : side] = pick(middle_ref, 0, side - 2 * MARGIN)
                ref[s, :, side : side + MARGIN] = lax.select(col_even, inner, outer)


def placed_flows(meta_ref, prior_ref, order_ref, lag_ref, cross_ref, first_ref, second_ref, s, shape, sizes):
    size_gz, size_row, size_col, sec_count, per_side = sizes
    place_count = per_side * per_side
    lanes_each = 2 * size_gz * sec_count * size_col * per_side
    row_count = size_row * per_side
    rows_each = row_count // size_row
    holder = lax.broadcasted_iota(jnp.int32, shape, 0)
    lane = lax.broadcasted_iota(jnp.int32, shape, 1)
    slot = jnp.zeros(shape, jnp.int32)
    for m in range(row_count):
        here = jnp.logical_and(holder == m // rows_each, lane // lanes_each == m % rows_each)
        slot = jnp.where(here, order_ref[m], slot)
    lane = lane % lanes_each
    my_gz, my_row, my_col = meta_ref[0], meta_ref[1], meta_ref[2]
    total_out = jnp.zeros(shape, jnp.float32)
    scale = 2.0 / float(PATCH) ** 3
    down = (lax.broadcasted_iota(jnp.int32, (LAGS, LAGS), 0) - LAGS // 2).astype(jnp.float32)
    across = (lax.broadcasted_iota(jnp.int32, (LAGS, LAGS), 1) - LAGS // 2).astype(jnp.float32)
    for n in range(place_count):
        pi, pj = n // per_side, n % per_side
        cross_parts(first_ref.at[n], second_ref.at[n], cross_ref)
        p = prior_ref[0, s, pi, pj]
        q = prior_ref[1, s, pi, pj]
        row_lags = lag_rows(lag_ref, p)
        col_lags = lag_rows(lag_ref, q)
        half = lax.dot_general(
            cross_ref[...], col_lags, (((1,), (1,)), ((), ())), preferred_element_type=jnp.float32
        ).astype(jnp.bfloat16)
        surface = jnp.dot(row_lags, half, preferred_element_type=jnp.float32) * scale
        weights = surface * surface
        total = 1.0 + jnp.sum(weights, keepdims=True)
        shift_r = jnp.sum(weights * down, keepdims=True) / total
        shift_c = jnp.sum(weights * across, keepdims=True) / total
        mine = slot == my_row * per_side + pi
        place = (my_gz * sec_count + s) * (size_col * per_side) + my_col * per_side + pj
        half_lanes = lanes_each // 2
        total_out += jnp.where(jnp.logical_and(mine, lane == place), p.astype(jnp.float32) + shift_r, 0.0)
        total_out += jnp.where(jnp.logical_and(mine, lane == place + half_lanes), q.astype(jnp.float32) + shift_c, 0.0)
    return total_out


def first_kernel(
    meta_ref, table_ref, turned_ref, own_ref, col_inner_ref, col_outer_ref, row_inner_ref, row_outer_ref,
    part_ref, ext_ref, rows_ref, spec_ref, *, section,
):
    pieces = ((own_ref,), (col_inner_ref, col_outer_ref), (row_inner_ref, row_outer_ref))
    fill_parts(table_ref, turned_ref, meta_ref, pieces, section, part_ref, ext_ref, rows_ref, spec_ref)


def next_kernel(
    meta_ref, prior_ref, order_ref, table_ref, turned_ref, own_ref, col_inner_ref, col_outer_ref, row_inner_ref, row_outer_ref,
    lag_ref, flow_in_ref, before_ref, part_ref, flow_ref, ext_ref, rows_ref, spec_ref, cross_ref, *, section, sizes,
):
    pieces = ((own_ref,), (col_inner_ref, col_outer_ref), (row_inner_ref, row_outer_ref))
    fill_parts(table_ref, turned_ref, meta_ref, pieces, section, part_ref, ext_ref, rows_ref, spec_ref)
    flow_ref[...] = flow_in_ref[...] + placed_flows(
        meta_ref, prior_ref, order_ref, lag_ref, cross_ref, before_ref, part_ref, section - 1, flow_ref.shape, sizes
    )


def last_kernel(
    meta_ref, prior_ref, order_ref, table_ref, turned_ref, lag_ref, middle_ref, first_inner_ref, first_outer_ref, col_inner_ref, col_outer_ref,
    row_inner_ref, row_outer_ref, flow_ref, first_ref, out_ref, ext_ref, rows_ref, spec_ref, part_ref, cross_ref, *, sizes,
):
    size_gz, size_row, size_col, sec_count, _ = sizes
    center = (middle_ref, first_inner_ref, first_outer_ref)
    pieces = (center, (col_inner_ref, col_outer_ref), (row_inner_ref, row_outer_ref))
    fill_parts(table_ref, turned_ref, meta_ref, pieces, 0, part_ref, ext_ref, rows_ref, spec_ref)
    flow = flow_ref[...] + placed_flows(
        meta_ref, prior_ref, order_ref, lag_ref, cross_ref, first_ref, part_ref, sec_count - 1, flow_ref.shape, sizes
    )
    for g in range(size_gz):
        for r in range(size_row):
            out_ref[(g * size_row + r) * size_col : (g * size_row + r + 1) * size_col, :] = jnp.broadcast_to(
                flow[r : r + 1, :], (size_col, flow.shape[1])
            )


def exchanges(size):
    inner = [(i, i + 1) for i in range(0, size - 1, 2)]
    outer = [(i, i + 1) for i in range(1, size - 1, 2)]
    return [pairs + [(j, i) for i, j in pairs] for pairs in (inner, outer)]


def match(sections, priors, row_order):
    sec_count, side = sections.shape[:2]
    per_side = side // STRIDE
    place_count = per_side * per_side
    size_gz, size_row, size_col = (lax.axis_size(a) for a in AXES)
    table, lag_table = frequency_tables()
    turned = jnp.asarray(table.T).astype(jnp.bfloat16)
    table = jnp.asarray(table).astype(jnp.bfloat16)
    lag_table = jnp.asarray(np.stack(np.split(lag_table, PATCH // 128, axis=1))).astype(jnp.bfloat16).astype(jnp.float32)
    meta = jnp.stack([lax.axis_index(a) for a in AXES]).astype(jnp.int32)
    wide = side + HALO
    vmem = pl.BlockSpec(memory_space=pltpu.VMEM)
    smem = pl.BlockSpec(memory_space=pltpu.SMEM)
    params = pltpu.CompilerParams(vmem_limit_bytes=VMEM_LIMIT)
    small = pltpu.CompilerParams(vmem_limit_bytes=VMEM_LIMIT // 4)

    def pixels(*shape):
        return jax.ShapeDtypeStruct(shape, jnp.bfloat16)

    gz_pairs = [(i, (i - 1) % size_gz) for i in range(size_gz)]
    col_inner, col_outer = exchanges(size_col)
    row_inner, row_outer = exchanges(size_row)
    glue_cost = pl.CostEstimate(flops=GLUE_FLOPS, bytes_accessed=0, transcendentals=0)
    cuts = pl.pallas_call(
        cut_kernel,
        out_shape=[pixels(sec_count, side, MARGIN)] * 2 + [pixels(1, side, MARGIN)] * 2 + [pixels(1, side, side - HALO), pixels(*sections.shape)],
        in_specs=[smem, vmem],
        out_specs=[vmem] * 6,
        compiler_params=small,
        cost_estimate=glue_cost,
        name="cut",
    )(meta, sections)
    own = cuts[5]
    own_cols = (lax.ppermute(cuts[0], "col", col_inner), lax.ppermute(cuts[1], "col", col_outer))
    first_inner = lax.ppermute(cuts[2], "gz", gz_pairs)
    first_outer = lax.ppermute(cuts[3], "gz", gz_pairs)
    middle = lax.ppermute(cuts[4], "gz", gz_pairs)
    last_cols = (lax.ppermute(first_inner, "col", col_inner), lax.ppermute(first_outer, "col", col_outer))

    def edges(count, center, cols):
        call = pl.pallas_call(
            edge_kernel,
            out_shape=[pixels(count, MARGIN, wide)] * 2,
            in_specs=[smem] + [vmem] * (len(center) + 2),
            out_specs=[vmem] * 2,
            compiler_params=small,
            cost_estimate=glue_cost,
        )
        inner, outer = call(meta, *center, *cols)
        return lax.ppermute(inner, "row", row_inner), lax.ppermute(outer, "row", row_outer)

    last_center = (middle, first_inner, first_outer)
    own_rows = edges(sec_count, (own,), own_cols)
    last_rows = edges(1, last_center, last_cols)
    lanes = (row_order.shape[0] // size_row) * 2 * size_gz * sec_count * size_col * per_side
    devices = size_gz * size_row * size_col
    sizes = (size_gz, size_row, size_col, sec_count, per_side)
    parts = (place_count, 4, HALF, HALF)

    part_shape = jax.ShapeDtypeStruct(parts, jnp.float32)
    flow_shape = jax.ShapeDtypeStruct((size_row, lanes), jnp.float32)
    ext_scratch = pltpu.VMEM((wide, wide), jnp.bfloat16)
    rows_scratch = pltpu.VMEM((wide, PATCH), jnp.bfloat16)
    spec_scratch = pltpu.VMEM((PATCH, PATCH), jnp.float32)
    part_scratch = pltpu.VMEM(parts, jnp.float32)
    cross_scratch = pltpu.VMEM((PATCH, PATCH), jnp.bfloat16)
    spectra_cost = 2 * per_side * wide * PATCH * PATCH + 2 * place_count * PATCH**3
    pair_cost = 2 * place_count * PATCH * LAGS * (PATCH + LAGS)

    def cost(flops):
        return pl.CostEstimate(flops=flops, bytes_accessed=place_count * PATCH * PATCH * 4, transcendentals=0)

    flow = jnp.zeros((size_row, lanes), jnp.float32)
    pieces = (own, *own_cols, *own_rows)
    first_call = pl.pallas_call(
        functools.partial(first_kernel, section=0),
        out_shape=part_shape,
        in_specs=[smem] + [vmem] * 7,
        out_specs=vmem,
        scratch_shapes=[ext_scratch, rows_scratch, spec_scratch],
        compiler_params=params,
        cost_estimate=cost(spectra_cost),
        name="first",
    )
    part = first_call(meta, table, turned, *pieces)
    for section in range(1, sec_count):
        next_call = pl.pallas_call(
            functools.partial(next_kernel, section=section, sizes=sizes),
            out_shape=(part_shape, flow_shape),
            in_specs=[smem] * 3 + [vmem] * 10,
            out_specs=(vmem, vmem),
            scratch_shapes=[ext_scratch, rows_scratch, spec_scratch, cross_scratch],
            compiler_params=params,
            cost_estimate=cost(spectra_cost + pair_cost),
            name="next",
        )
        part, flow = next_call(meta, priors, row_order, table, turned, *pieces, lag_table, flow, part)
    sent = pl.pallas_call(
        functools.partial(last_kernel, sizes=sizes),
        out_shape=jax.ShapeDtypeStruct((devices, lanes), jnp.float32),
        in_specs=[smem] * 3 + [vmem] * 12,
        out_specs=vmem,
        scratch_shapes=[ext_scratch, rows_scratch, spec_scratch, part_scratch, cross_scratch],
        compiler_params=params,
        cost_estimate=cost(spectra_cost + pair_cost),
        name="last",
    )(meta, priors, row_order, table, turned, lag_table, *last_center, *last_cols, *last_rows, flow, part)
    received = lax.all_to_all(sent, AXES, 0, 0, tiled=True)
    return jnp.sum(received, axis=0).reshape(row_order.shape[0] // size_row, -1)


def solution(mesh):
    placed = (P("gz", "row", "col"), P(None, "gz", "row", "col"), P())
    return jax.shard_map(match, mesh=mesh, in_specs=placed, out_specs=P("row", None), check_vma=False)
```

```python
import functools
import math

import jax
import jax.numpy as jnp
import numpy as np
from jax import lax
from jax.experimental import pallas as pl
from jax.experimental.pallas import tpu as pltpu
from jax.sharding import PartitionSpec as P


PATCH = 512
STRIDE = 256
LAGS = 128
MAXOFF = 64
HALO = 256
HALF = PATCH // 2
MARGIN = HALO // 2
AXES = ("gz", "row", "col")
VMEM_LIMIT = 16 * 1024 * 1024
GLUE_FLOPS = 4 * 10**9


def frequency_tables():
    frequencies = np.concatenate([np.arange(0, HALF, 2), np.arange(1, HALF, 2)])[:, None]
    places = np.arange(PATCH)[None, :]
    step = 2.0 * math.pi / PATCH
    cosine = np.cos(np.mod(frequencies * places, PATCH) * step)
    sine_part = np.sin(np.mod(frequencies * places, PATCH) * step)
    sine_part[0] = np.cos(np.mod(HALF * places[0], PATCH) * step)
    quarter = HALF // 2
    table = np.concatenate([cosine[:quarter], sine_part[:quarter], cosine[quarter:], sine_part[quarter:]], axis=0)
    lags = np.arange(-MAXOFF - LAGS // 2, MAXOFF + LAGS // 2) % PATCH
    return table[:, :HALF].astype(np.float32), table.T[lags].astype(np.float32)


def blocks():
    quarter = HALF // 2
    for k_odd in range(2):
        for l_odd in range(2):
            cols = slice(l_odd * HALF, l_odd * HALF + quarter)
            if k_odd == 0:
                yield slice(0, 16), cols
                yield slice(16, quarter), cols
            else:
                yield slice(HALF, HALF + quarter), cols


def sines(part):
    return slice(part.start + HALF // 2, part.stop + HALF // 2)


def split_parts(spec_ref, out_ref):
    for rows, cols in blocks():
        cc = spec_ref[rows, cols]
        cs = spec_ref[rows, sines(cols)]
        sc = spec_ref[sines(rows), cols]
        ss = spec_ref[sines(rows), sines(cols)]
        a, b, c, d = cc - ss, sc + cs, cc + ss, sc - cs
        if cols.start == 0:
            edge = lax.broadcasted_iota(jnp.int32, cc.shape, 1) == 0
            a, b, c, d = jnp.where(edge, cc, a), jnp.where(edge, sc, b), jnp.where(edge, cs, c), jnp.where(edge, ss, d)
        if rows.start == 0:
            edge = lax.broadcasted_iota(jnp.int32, cc.shape, 0) == 0
            a, b, c, d = jnp.where(edge, cc, a), jnp.where(edge, cs, b), jnp.where(edge, sc, c), jnp.where(edge, ss, d)
        out_ref[rows, cols] = a
        out_ref[rows, sines(cols)] = b
        out_ref[sines(rows), cols] = c
        out_ref[sines(rows), sines(cols)] = d


def cross_parts(first_ref, second_ref, out_ref):
    for rows, cols in blocks():
        places = ((rows, cols), (rows, sines(cols)), (sines(rows), cols), (sines(rows), sines(cols)))
        a, b, c, d = (first_ref[place] for place in places)
        e, f, g, h = (second_ref[place] for place in places)
        p, u = a * e + b * f, a * f - b * e
        q, v = c * g + d * h, c * h - d * g
        cc, cs, sc, ss = p + q, u - v, u + v, q - p
        if cols.start == 0:
            edge = lax.broadcasted_iota(jnp.int32, cc.shape, 1) == 0
            cc, cs, sc, ss = jnp.where(edge, p, cc), jnp.where(edge, q, cs), jnp.where(edge, u, sc), jnp.where(edge, v, ss)
        if rows.start == 0:
            row = lax.broadcasted_iota(jnp.int32, cc.shape, 0) == 0
            cc, cs, sc, ss = jnp.where(row, p, cc), jnp.where(row, u, cs), jnp.where(row, q, sc), jnp.where(row, v, ss)
            if cols.start == 0:
                corner = jnp.logical_and(row, edge)
                cc, cs = jnp.where(corner, 0.5 * (a * e), cc), jnp.where(corner, 0.5 * (b * f), cs)
                sc, ss = jnp.where(corner, 0.5 * (c * g), sc), jnp.where(corner, 0.5 * (d * h), ss)
        for place, value in zip(places, (cc, cs, sc, ss)):
            out_ref[place] = value.astype(jnp.bfloat16)


def lag_rows(lag_ref, offset):
    pieces = [lag_ref[n, pl.ds(offset + MAXOFF, LAGS), :] for n in range(lag_ref.shape[0])]
    return jnp.concatenate(pieces, axis=1).astype(jnp.bfloat16)


def fill_parts(table_ref, turned_ref, meta_ref, pieces, s, out_ref, ext_ref, rows_ref, spec_ref):
    center_refs, col_refs, row_refs = pieces
    top = ext_ref.shape[0] - MARGIN
    row_even, col_even = meta_ref[1] % 2 == 0, meta_ref[2] % 2 == 0
    inner, outer = row_refs[0][s], row_refs[1][s]
    ext_ref[0:MARGIN, :] = lax.select(row_even, outer, inner)
    ext_ref[top:, :] = lax.select(row_even, inner, outer)
    inner, outer = col_refs[0][s], col_refs[1][s]
    ext_ref[MARGIN:top, 0:MARGIN] = lax.select(col_even, outer, inner)
    ext_ref[MARGIN:top, top:] = lax.select(col_even, inner, outer)
    center_rows(ext_ref.at[MARGIN:top, MARGIN:top], col_even, center_refs, s, slice(0, top - MARGIN))
    per_side = (top - MARGIN) // STRIDE
    parities = (slice(0, HALF), slice(HALF, PATCH))
    for pj in range(per_side):
        near = ext_ref[:, pj * STRIDE : pj * STRIDE + HALF]
        away = ext_ref[:, pj * STRIDE + HALF : pj * STRIDE + PATCH]
        for part, folded in zip(parities, (near + away, near - away)):
            rows_ref[pj, :, part] = jnp.dot(folded, turned_ref[:, part], preferred_element_type=jnp.float32).astype(jnp.bfloat16)
        for pi in range(per_side):
            n = pi * per_side + pj
            near = rows_ref[pj, pi * STRIDE : pi * STRIDE + HALF, :]
            away = rows_ref[pj, pi * STRIDE + HALF : pi * STRIDE + PATCH, :]
            for part, folded in zip(parities, (near + away, near - away)):
                spec_ref[n % 2, part] = jnp.dot(table_ref[part], folded, preferred_element_type=jnp.float32)
            split_parts(spec_ref.at[n % 2], out_ref.at[n])


def center_rows(out_ref, col_even, center_refs, s, rows):
    if len(center_refs) == 1:
        out_ref[...] = center_refs[0][s, rows]
        return
    middle_ref, inner_ref, outer_ref = center_refs
    side = out_ref.shape[1]
    inner, outer = inner_ref[s, rows], outer_ref[s, rows]
    out_ref[:, 0:MARGIN] = lax.select(col_even, outer, inner)
    out_ref[:, MARGIN : side - MARGIN] = middle_ref[s, rows]
    out_ref[:, side - MARGIN :] = lax.select(col_even, inner, outer)


def cut_kernel(meta_ref, far_ref, inner_ref, outer_ref, first_inner_ref, first_outer_ref, middle_ref, own_ref):
    own_ref[...] = far_ref[...]
    side = own_ref.shape[2]
    col_even = meta_ref[2] % 2 == 0
    for s in range(own_ref.shape[0]):
        low, high = own_ref[s, :, 0:MARGIN], own_ref[s, :, side - MARGIN :]
        inner_ref[s] = lax.select(col_even, high, low)
        outer_ref[s] = lax.select(col_even, low, high)
    low, high = own_ref[0, :, 0:MARGIN], own_ref[0, :, side - MARGIN :]
    first_inner_ref[0] = lax.select(col_even, high, low)
    first_outer_ref[0] = lax.select(col_even, low, high)
    middle_ref[0] = own_ref[0, :, MARGIN : side - MARGIN]


def edge_kernel(meta_ref, *refs):
    *center_refs, col_inner_ref, col_outer_ref, inner_ref, outer_ref = refs
    side = col_inner_ref.shape[1]
    row_even, col_even = meta_ref[1] % 2 == 0, meta_ref[2] % 2 == 0
    low, high = slice(0, MARGIN), slice(side - MARGIN, side)
    for s in range(inner_ref.shape[0]):
        for ref, even_rows, odd_rows in ((inner_ref, high, low), (outer_ref, low, high)):
            def pick(source, start, stop):
                return lax.select(row_even, source[s, even_rows, start:stop], source[s, odd_rows, start:stop])

            inner, outer = pick(col_inner_ref, 0, MARGIN), pick(col_outer_ref, 0, MARGIN)
            ref[s, :, 0:MARGIN] = lax.select(col_even, outer, inner)
            ref[s, :, side + MARGIN :] = lax.select(col_even, inner, outer)
            if len(center_refs) == 1:
                ref[s, :, MARGIN : side + MARGIN] = pick(center_refs[0], 0, side)
            else:
                middle_ref, first_inner_ref, first_outer_ref = center_refs
                inner, outer = pick(first_inner_ref, 0, MARGIN), pick(first_outer_ref, 0, MARGIN)
                ref[s, :, MARGIN : 2 * MARGIN] = lax.select(col_even, outer, inner)
                ref[s, :, 2 * MARGIN : side] = pick(middle_ref, 0, side - 2 * MARGIN)
                ref[s, :, side : side + MARGIN] = lax.select(col_even, inner, outer)


def placed_flows(meta_ref, prior_ref, order_ref, lag_ref, cross_ref, first_ref, second_ref, s, shape, sizes):
    size_gz, size_row, size_col, sec_count, per_side = sizes
    place_count = per_side * per_side
    lanes_each = 2 * size_gz * sec_count * size_col * per_side
    row_count = size_row * per_side
    rows_each = row_count // size_row
    holder = lax.broadcasted_iota(jnp.int32, shape, 0)
    lane = lax.broadcasted_iota(jnp.int32, shape, 1)
    slot = jnp.zeros(shape, jnp.int32)
    for m in range(row_count):
        here = jnp.logical_and(holder == m // rows_each, lane // lanes_each == m % rows_each)
        slot = jnp.where(here, order_ref[m], slot)
    lane = lane % lanes_each
    my_gz, my_row, my_col = meta_ref[0], meta_ref[1], meta_ref[2]
    total_out = jnp.zeros(shape, jnp.float32)
    scale = 2.0 / float(PATCH) ** 3
    down = (lax.broadcasted_iota(jnp.int32, (LAGS, LAGS), 0) - LAGS // 2).astype(jnp.float32)
    across = (lax.broadcasted_iota(jnp.int32, (1, LAGS), 1) - LAGS // 2).astype(jnp.float32)
    sums = []
    for n in range(place_count):
        pi, pj = n // per_side, n % per_side
        cross_parts(first_ref.at[n], second_ref.at[n], cross_ref.at[n])
        row_lags = lag_rows(lag_ref, prior_ref[0, s, pi, pj])
        col_lags = lag_rows(lag_ref, prior_ref[1, s, pi, pj])
        half = jnp.dot(row_lags, cross_ref[n], preferred_element_type=jnp.float32).astype(jnp.bfloat16)
        surface = scale * lax.dot_general(
            half, col_lags, (((1,), (1,)), ((), ())), preferred_element_type=jnp.float32
        )
        weights = surface * surface
        plain = jnp.sum(weights, axis=0, keepdims=True)
        sums += [plain, jnp.sum(weights * down, axis=0, keepdims=True), plain * across]
    sums = jnp.sum(jnp.concatenate(sums, axis=0), axis=1, keepdims=True)
    for n in range(place_count):
        pi, pj = n // per_side, n % per_side
        total = 1.0 + sums[3 * n : 3 * n + 1]
        place = (my_gz * sec_count + s) * (size_col * per_side) + my_col * per_side + pj
        for c in range(2):
            value = prior_ref[c, s, pi, pj].astype(jnp.float32) + sums[3 * n + 1 + c : 3 * n + 2 + c] / total
            here = jnp.logical_and(slot == my_row * per_side + pi, lane == place + c * (lanes_each // 2))
            total_out += jnp.where(here, value, 0.0)
    return total_out


def first_kernel(
    meta_ref, table_ref, turned_ref, own_ref, col_inner_ref, col_outer_ref, row_inner_ref, row_outer_ref,
    part_ref, ext_ref, rows_ref, spec_ref, *, section,
):
    pieces = ((own_ref,), (col_inner_ref, col_outer_ref), (row_inner_ref, row_outer_ref))
    fill_parts(table_ref, turned_ref, meta_ref, pieces, section, part_ref, ext_ref, rows_ref, spec_ref)


def next_kernel(
    meta_ref, prior_ref, order_ref, table_ref, turned_ref, own_ref, col_inner_ref, col_outer_ref, row_inner_ref, row_outer_ref,
    lag_ref, flow_in_ref, before_ref, part_ref, flow_ref, ext_ref, rows_ref, spec_ref, cross_ref, *, section, sizes,
):
    pieces = ((own_ref,), (col_inner_ref, col_outer_ref), (row_inner_ref, row_outer_ref))
    fill_parts(table_ref, turned_ref, meta_ref, pieces, section, part_ref, ext_ref, rows_ref, spec_ref)
    flow_ref[...] = flow_in_ref[...] + placed_flows(
        meta_ref, prior_ref, order_ref, lag_ref, cross_ref, before_ref, part_ref, section - 1, flow_ref.shape, sizes
    )


def last_kernel(
    meta_ref, prior_ref, order_ref, table_ref, turned_ref, lag_ref, middle_ref, first_inner_ref, first_outer_ref, col_inner_ref, col_outer_ref,
    row_inner_ref, row_outer_ref, flow_ref, first_ref, out_ref, ext_ref, rows_ref, spec_ref, part_ref, cross_ref, *, sizes,
):
    size_gz, size_row, size_col, sec_count, _ = sizes
    center = (middle_ref, first_inner_ref, first_outer_ref)
    pieces = (center, (col_inner_ref, col_outer_ref), (row_inner_ref, row_outer_ref))
    fill_parts(table_ref, turned_ref, meta_ref, pieces, 0, part_ref, ext_ref, rows_ref, spec_ref)
    flow = flow_ref[...] + placed_flows(
        meta_ref, prior_ref, order_ref, lag_ref, cross_ref, first_ref, part_ref, sec_count - 1, flow_ref.shape, sizes
    )
    for g in range(size_gz):
        for r in range(size_row):
            out_ref[(g * size_row + r) * size_col : (g * size_row + r + 1) * size_col, :] = jnp.broadcast_to(
                flow[r : r + 1, :], (size_col, flow.shape[1])
            )


def exchanges(size):
    inner = [(i, i + 1) for i in range(0, size - 1, 2)]
    outer = [(i, i + 1) for i in range(1, size - 1, 2)]
    return [pairs + [(j, i) for i, j in pairs] for pairs in (inner, outer)]


def match(sections, priors, row_order):
    sec_count, side = sections.shape[:2]
    per_side = side // STRIDE
    place_count = per_side * per_side
    size_gz, size_row, size_col = (lax.axis_size(a) for a in AXES)
    table, lag_table = frequency_tables()
    turned = jnp.asarray(table.T).astype(jnp.bfloat16)
    table = jnp.asarray(table).astype(jnp.bfloat16)
    lag_table = jnp.asarray(np.stack(np.split(lag_table, PATCH // 128, axis=1))).astype(jnp.bfloat16).astype(jnp.float32)
    meta = jnp.stack([lax.axis_index(a) for a in AXES]).astype(jnp.int32)
    wide = side + HALO
    vmem = pl.BlockSpec(memory_space=pltpu.VMEM)
    smem = pl.BlockSpec(memory_space=pltpu.SMEM)
    params = pltpu.CompilerParams(vmem_limit_bytes=VMEM_LIMIT)
    small = pltpu.CompilerParams(vmem_limit_bytes=VMEM_LIMIT // 4)

    def pixels(*shape):
        return jax.ShapeDtypeStruct(shape, jnp.bfloat16)

    gz_pairs = [(i, (i - 1) % size_gz) for i in range(size_gz)]
    col_inner, col_outer = exchanges(size_col)
    row_inner, row_outer = exchanges(size_row)
    glue_cost = pl.CostEstimate(flops=GLUE_FLOPS, bytes_accessed=0, transcendentals=0)
    cuts = pl.pallas_call(
        cut_kernel,
        out_shape=[pixels(sec_count, side, MARGIN)] * 2 + [pixels(1, side, MARGIN)] * 2 + [pixels(1, side, side - HALO), pixels(*sections.shape)],
        in_specs=[smem, vmem],
        out_specs=[vmem] * 6,
        compiler_params=small,
        cost_estimate=glue_cost,
        name="cut",
    )(meta, sections)
    own = cuts[5]
    own_cols = (lax.ppermute(cuts[0], "col", col_inner), lax.ppermute(cuts[1], "col", col_outer))
    first_inner = lax.ppermute(cuts[2], "gz", gz_pairs)
    first_outer = lax.ppermute(cuts[3], "gz", gz_pairs)
    middle = lax.ppermute(cuts[4], "gz", gz_pairs)
    last_cols = (lax.ppermute(first_inner, "col", col_inner), lax.ppermute(first_outer, "col", col_outer))

    def edges(count, center, cols):
        call = pl.pallas_call(
            edge_kernel,
            out_shape=[pixels(count, MARGIN, wide)] * 2,
            in_specs=[smem] + [vmem] * (len(center) + 2),
            out_specs=[vmem] * 2,
            compiler_params=small,
            cost_estimate=glue_cost,
        )
        inner, outer = call(meta, *center, *cols)
        return lax.ppermute(inner, "row", row_inner), lax.ppermute(outer, "row", row_outer)

    last_center = (middle, first_inner, first_outer)
    own_rows = edges(sec_count, (own,), own_cols)
    last_rows = edges(1, last_center, last_cols)
    lanes = (row_order.shape[0] // size_row) * 2 * size_gz * sec_count * size_col * per_side
    devices = size_gz * size_row * size_col
    sizes = (size_gz, size_row, size_col, sec_count, per_side)
    parts = (place_count, PATCH, PATCH)

    part_shape = jax.ShapeDtypeStruct(parts, jnp.float32)
    flow_shape = jax.ShapeDtypeStruct((size_row, lanes), jnp.float32)
    ext_scratch = pltpu.VMEM((wide, wide), jnp.bfloat16)
    rows_scratch = pltpu.VMEM((per_side, wide, PATCH), jnp.bfloat16)
    spec_scratch = pltpu.VMEM((2, PATCH, PATCH), jnp.float32)
    part_scratch = pltpu.VMEM(parts, jnp.float32)
    cross_scratch = pltpu.VMEM((place_count, PATCH, PATCH), jnp.bfloat16)
    spectra_cost = 2 * per_side * wide * PATCH * PATCH + 2 * place_count * PATCH**3
    pair_cost = 2 * place_count * PATCH * LAGS * (PATCH + LAGS)

    def cost(flops):
        return pl.CostEstimate(flops=flops, bytes_accessed=place_count * PATCH * PATCH * 4, transcendentals=0)

    flow = jnp.zeros((size_row, lanes), jnp.float32)
    pieces = (own, *own_cols, *own_rows)
    first_call = pl.pallas_call(
        functools.partial(first_kernel, section=0),
        out_shape=part_shape,
        in_specs=[smem] + [vmem] * 7,
        out_specs=vmem,
        scratch_shapes=[ext_scratch, rows_scratch, spec_scratch],
        compiler_params=params,
        cost_estimate=cost(spectra_cost),
        name="first",
    )
    part = first_call(meta, table, turned, *pieces)
    for section in range(1, sec_count):
        next_call = pl.pallas_call(
            functools.partial(next_kernel, section=section, sizes=sizes),
            out_shape=(part_shape, flow_shape),
            in_specs=[smem] * 3 + [vmem] * 10,
            out_specs=(vmem, vmem),
            scratch_shapes=[ext_scratch, rows_scratch, spec_scratch, cross_scratch],
            compiler_params=params,
            cost_estimate=cost(spectra_cost + pair_cost),
            name="next",
        )
        part, flow = next_call(meta, priors, row_order, table, turned, *pieces, lag_table, flow, part)
    sent = pl.pallas_call(
        functools.partial(last_kernel, sizes=sizes),
        out_shape=jax.ShapeDtypeStruct((devices, lanes), jnp.float32),
        in_specs=[smem] * 3 + [vmem] * 12,
        out_specs=vmem,
        scratch_shapes=[ext_scratch, rows_scratch, spec_scratch, part_scratch, cross_scratch],
        compiler_params=params,
        cost_estimate=cost(spectra_cost + pair_cost),
        name="last",
    )(meta, priors, row_order, table, turned, lag_table, *last_center, *last_cols, *last_rows, flow, part)
    received = lax.all_to_all(sent, AXES, 0, 0, tiled=True)
    return jnp.sum(received, axis=0).reshape(row_order.shape[0] // size_row, -1)


def solution(mesh):
    placed = (P("gz", "row", "col"), P(None, "gz", "row", "col"), P())
    return jax.shard_map(match, mesh=mesh, in_specs=placed, out_specs=P("row", None), check_vma=False)
```

```python
import functools
import math

import jax
import jax.numpy as jnp
import numpy as np
from jax import lax
from jax.experimental import pallas as pl
from jax.experimental.pallas import tpu as pltpu
from jax.sharding import PartitionSpec as P


PATCH = 512
STRIDE = 256
LAGS = 128
MAXOFF = 64
HALO = 256
HALF = PATCH // 2
MARGIN = HALO // 2
AXES = ("gz", "row", "col")
VMEM_LIMIT = 16 * 1024 * 1024
GLUE_FLOPS = 4 * 10**9


def frequency_tables():
    frequencies = np.concatenate([np.arange(0, HALF, 2), np.arange(1, HALF, 2)])[:, None]
    places = np.arange(PATCH)[None, :]
    step = 2.0 * math.pi / PATCH
    cosine = np.cos(np.mod(frequencies * places, PATCH) * step)
    sine_part = np.sin(np.mod(frequencies * places, PATCH) * step)
    sine_part[0] = np.cos(np.mod(HALF * places[0], PATCH) * step)
    quarter = HALF // 2
    table = np.concatenate([cosine[:quarter], sine_part[:quarter], cosine[quarter:], sine_part[quarter:]], axis=0)
    lags = np.arange(-MAXOFF - LAGS // 2, MAXOFF + LAGS // 2) % PATCH
    return table[:, :HALF].astype(np.float32), table.T[lags].astype(np.float32)


def blocks():
    quarter = HALF // 2
    for k_odd in range(2):
        for l_odd in range(2):
            cols = slice(l_odd * HALF, l_odd * HALF + quarter)
            if k_odd == 0:
                yield slice(0, 16), cols
                yield slice(16, quarter), cols
            else:
                yield slice(HALF, HALF + quarter), cols


def sines(part):
    return slice(part.start + HALF // 2, part.stop + HALF // 2)


def split_parts(spec_ref, out_ref):
    for rows, cols in blocks():
        cc = spec_ref[rows, cols]
        cs = spec_ref[rows, sines(cols)]
        sc = spec_ref[sines(rows), cols]
        ss = spec_ref[sines(rows), sines(cols)]
        a, b, c, d = cc - ss, sc + cs, cc + ss, sc - cs
        if cols.start == 0:
            edge = lax.broadcasted_iota(jnp.int32, cc.shape, 1) == 0
            a, b, c, d = jnp.where(edge, cc, a), jnp.where(edge, sc, b), jnp.where(edge, cs, c), jnp.where(edge, ss, d)
        if rows.start == 0:
            edge = lax.broadcasted_iota(jnp.int32, cc.shape, 0) == 0
            a, b, c, d = jnp.where(edge, cc, a), jnp.where(edge, cs, b), jnp.where(edge, sc, c), jnp.where(edge, ss, d)
        out_ref[rows, cols] = a
        out_ref[rows, sines(cols)] = b
        out_ref[sines(rows), cols] = c
        out_ref[sines(rows), sines(cols)] = d


def cross_parts(first_ref, second_ref, out_ref):
    for rows, cols in blocks():
        places = ((rows, cols), (rows, sines(cols)), (sines(rows), cols), (sines(rows), sines(cols)))
        a, b, c, d = (first_ref[place] for place in places)
        e, f, g, h = (second_ref[place] for place in places)
        p, u = a * e + b * f, a * f - b * e
        q, v = c * g + d * h, c * h - d * g
        cc, cs, sc, ss = p + q, u - v, u + v, q - p
        if cols.start == 0:
            edge = lax.broadcasted_iota(jnp.int32, cc.shape, 1) == 0
            cc, cs, sc, ss = jnp.where(edge, p, cc), jnp.where(edge, q, cs), jnp.where(edge, u, sc), jnp.where(edge, v, ss)
        if rows.start == 0:
            row = lax.broadcasted_iota(jnp.int32, cc.shape, 0) == 0
            cc, cs, sc, ss = jnp.where(row, p, cc), jnp.where(row, u, cs), jnp.where(row, q, sc), jnp.where(row, v, ss)
            if cols.start == 0:
                corner = jnp.logical_and(row, edge)
                cc, cs = jnp.where(corner, 0.5 * (a * e), cc), jnp.where(corner, 0.5 * (b * f), cs)
                sc, ss = jnp.where(corner, 0.5 * (c * g), sc), jnp.where(corner, 0.5 * (d * h), ss)
        for place, value in zip(places, (cc, cs, sc, ss)):
            out_ref[place] = value.astype(jnp.bfloat16)


def lag_rows(lag_ref, offset):
    pieces = [lag_ref[n, pl.ds(offset + MAXOFF, LAGS), :] for n in range(lag_ref.shape[0])]
    return jnp.concatenate(pieces, axis=1).astype(jnp.bfloat16)


def fill_parts(table_ref, turned_ref, meta_ref, pieces, s, out_ref, ext_ref, rows_ref, spec_ref):
    center_refs, col_refs, row_refs = pieces
    top = ext_ref.shape[0] - MARGIN
    row_even, col_even = meta_ref[1] % 2 == 0, meta_ref[2] % 2 == 0
    if len(row_refs) == 2:
        spans = ((row_refs, slice(None), slice(None)),)
    else:
        corners = row_refs[2:]
        spans = (
            (row_refs[:2], slice(None), slice(MARGIN, top)),
            (corners, slice(0, MARGIN), slice(0, MARGIN)),
            (corners, slice(MARGIN, 2 * MARGIN), slice(top, top + MARGIN)),
        )
    for refs, source, target in spans:
        inner, outer = refs[0][s, :, source], refs[1][s, :, source]
        ext_ref[0:MARGIN, target] = lax.select(row_even, outer, inner)
        ext_ref[top:, target] = lax.select(row_even, inner, outer)
    inner, outer = col_refs[0][s], col_refs[1][s]
    ext_ref[MARGIN:top, 0:MARGIN] = lax.select(col_even, outer, inner)
    ext_ref[MARGIN:top, top:] = lax.select(col_even, inner, outer)
    center_rows(ext_ref.at[MARGIN:top, MARGIN:top], col_even, center_refs, s, slice(0, top - MARGIN))
    per_side = (top - MARGIN) // STRIDE
    parities = (slice(0, HALF), slice(HALF, PATCH))
    for pj in range(per_side):
        near = ext_ref[:, pj * STRIDE : pj * STRIDE + HALF]
        away = ext_ref[:, pj * STRIDE + HALF : pj * STRIDE + PATCH]
        for part, folded in zip(parities, (near + away, near - away)):
            rows_ref[pj, :, part] = jnp.dot(folded, turned_ref[:, part], preferred_element_type=jnp.float32).astype(jnp.bfloat16)
        for pi in range(per_side):
            n = pi * per_side + pj
            near = rows_ref[pj, pi * STRIDE : pi * STRIDE + HALF, :]
            away = rows_ref[pj, pi * STRIDE + HALF : pi * STRIDE + PATCH, :]
            for part, folded in zip(parities, (near + away, near - away)):
                spec_ref[n % 2, part] = jnp.dot(table_ref[part], folded, preferred_element_type=jnp.float32)
            split_parts(spec_ref.at[n % 2], out_ref.at[n])


def center_rows(out_ref, col_even, center_refs, s, rows):
    if len(center_refs) == 1:
        out_ref[...] = center_refs[0][s, rows]
        return
    middle_ref, inner_ref, outer_ref = center_refs
    side = out_ref.shape[1]
    inner, outer = inner_ref[s, rows], outer_ref[s, rows]
    out_ref[:, 0:MARGIN] = lax.select(col_even, outer, inner)
    out_ref[:, MARGIN : side - MARGIN] = middle_ref[s, rows]
    out_ref[:, side - MARGIN :] = lax.select(col_even, inner, outer)


def cut_kernel(
    meta_ref, far_ref, inner_ref, outer_ref, row_inner_ref, row_outer_ref, first_inner_ref, first_outer_ref, middle_ref, own_ref,
):
    own_ref[...] = far_ref[...]
    side = own_ref.shape[2]
    row_even, col_even = meta_ref[1] % 2 == 0, meta_ref[2] % 2 == 0
    for s in range(own_ref.shape[0]):
        low, high = own_ref[s, :, 0:MARGIN], own_ref[s, :, side - MARGIN :]
        inner_ref[s] = lax.select(col_even, high, low)
        outer_ref[s] = lax.select(col_even, low, high)
        low, high = own_ref[s, 0:MARGIN, :], own_ref[s, side - MARGIN :, :]
        row_inner_ref[s] = lax.select(row_even, high, low)
        row_outer_ref[s] = lax.select(row_even, low, high)
    low, high = own_ref[0, :, 0:MARGIN], own_ref[0, :, side - MARGIN :]
    first_inner_ref[0] = lax.select(col_even, high, low)
    first_outer_ref[0] = lax.select(col_even, low, high)
    middle_ref[0] = own_ref[0, :, MARGIN : side - MARGIN]


def edge_kernel(meta_ref, *refs):
    *center_refs, col_inner_ref, col_outer_ref, inner_ref, outer_ref = refs
    side, wide = col_inner_ref.shape[1], inner_ref.shape[2]
    row_even, col_even = meta_ref[1] % 2 == 0, meta_ref[2] % 2 == 0
    low, high = slice(0, MARGIN), slice(side - MARGIN, side)
    for s in range(inner_ref.shape[0]):
        for ref, even_rows, odd_rows in ((inner_ref, high, low), (outer_ref, low, high)):
            def pick(source):
                return lax.select(row_even, source[s, even_rows, :], source[s, odd_rows, :])

            inner, outer = pick(col_inner_ref), pick(col_outer_ref)
            ref[s, :, 0:MARGIN] = lax.select(col_even, outer, inner)
            ref[s, :, wide - MARGIN :] = lax.select(col_even, inner, outer)
            if center_refs:
                middle_ref, first_inner_ref, first_outer_ref = center_refs
                inner, outer = pick(first_inner_ref), pick(first_outer_ref)
                ref[s, :, MARGIN : 2 * MARGIN] = lax.select(col_even, outer, inner)
                ref[s, :, 2 * MARGIN : side] = pick(middle_ref)
                ref[s, :, side : side + MARGIN] = lax.select(col_even, inner, outer)


def placed_flows(meta_ref, prior_ref, order_ref, lag_ref, cross_ref, first_ref, second_ref, s, shape, sizes):
    size_gz, size_row, size_col, sec_count, per_side = sizes
    place_count = per_side * per_side
    lanes_each = 2 * size_gz * sec_count * size_col * per_side
    row_count = size_row * per_side
    rows_each = row_count // size_row
    holder = lax.broadcasted_iota(jnp.int32, shape, 0)
    lane = lax.broadcasted_iota(jnp.int32, shape, 1)
    slot = jnp.zeros(shape, jnp.int32)
    for m in range(row_count):
        here = jnp.logical_and(holder == m // rows_each, lane // lanes_each == m % rows_each)
        slot = jnp.where(here, order_ref[m], slot)
    lane = lane % lanes_each
    my_gz, my_row, my_col = meta_ref[0], meta_ref[1], meta_ref[2]
    total_out = jnp.zeros(shape, jnp.float32)
    scale = 2.0 / float(PATCH) ** 3
    down = (lax.broadcasted_iota(jnp.int32, (LAGS, LAGS), 0) - LAGS // 2).astype(jnp.float32)
    across = (lax.broadcasted_iota(jnp.int32, (1, LAGS), 1) - LAGS // 2).astype(jnp.float32)
    sums = []
    for n in range(place_count):
        pi, pj = n // per_side, n % per_side
        cross_parts(first_ref.at[n], second_ref.at[n], cross_ref.at[n])
        row_lags = lag_rows(lag_ref, prior_ref[0, s, pi, pj])
        col_lags = lag_rows(lag_ref, prior_ref[1, s, pi, pj])
        half = jnp.dot(row_lags, cross_ref[n], preferred_element_type=jnp.float32).astype(jnp.bfloat16)
        surface = scale * lax.dot_general(
            half, col_lags, (((1,), (1,)), ((), ())), preferred_element_type=jnp.float32
        )
        weights = surface * surface
        plain = jnp.sum(weights, axis=0, keepdims=True)
        sums += [plain, jnp.sum(weights * down, axis=0, keepdims=True), plain * across]
    sums = jnp.sum(jnp.concatenate(sums, axis=0), axis=1, keepdims=True)
    for n in range(place_count):
        pi, pj = n // per_side, n % per_side
        total = 1.0 + sums[3 * n : 3 * n + 1]
        place = (my_gz * sec_count + s) * (size_col * per_side) + my_col * per_side + pj
        for c in range(2):
            value = prior_ref[c, s, pi, pj].astype(jnp.float32) + sums[3 * n + 1 + c : 3 * n + 2 + c] / total
            here = jnp.logical_and(slot == my_row * per_side + pi, lane == place + c * (lanes_each // 2))
            total_out += jnp.where(here, value, 0.0)
    return total_out


def first_kernel(
    meta_ref, table_ref, turned_ref, own_ref, col_inner_ref, col_outer_ref, row_inner_ref, row_outer_ref,
    corner_inner_ref, corner_outer_ref, part_ref, ext_ref, rows_ref, spec_ref, *, section,
):
    pieces = ((own_ref,), (col_inner_ref, col_outer_ref), (row_inner_ref, row_outer_ref, corner_inner_ref, corner_outer_ref))
    fill_parts(table_ref, turned_ref, meta_ref, pieces, section, part_ref, ext_ref, rows_ref, spec_ref)


def next_kernel(
    meta_ref, prior_ref, order_ref, table_ref, turned_ref, own_ref, col_inner_ref, col_outer_ref, row_inner_ref, row_outer_ref,
    corner_inner_ref, corner_outer_ref, lag_ref, flow_in_ref, before_ref, part_ref, flow_ref, ext_ref, rows_ref, spec_ref, cross_ref, *, section, sizes,
):
    pieces = ((own_ref,), (col_inner_ref, col_outer_ref), (row_inner_ref, row_outer_ref, corner_inner_ref, corner_outer_ref))
    fill_parts(table_ref, turned_ref, meta_ref, pieces, section, part_ref, ext_ref, rows_ref, spec_ref)
    flow_ref[...] = flow_in_ref[...] + placed_flows(
        meta_ref, prior_ref, order_ref, lag_ref, cross_ref, before_ref, part_ref, section - 1, flow_ref.shape, sizes
    )


def last_kernel(
    meta_ref, prior_ref, order_ref, table_ref, turned_ref, lag_ref, middle_ref, first_inner_ref, first_outer_ref, col_inner_ref, col_outer_ref,
    row_inner_ref, row_outer_ref, flow_ref, first_ref, out_ref, ext_ref, rows_ref, spec_ref, part_ref, cross_ref, *, sizes,
):
    size_gz, size_row, size_col, sec_count, _ = sizes
    center = (middle_ref, first_inner_ref, first_outer_ref)
    pieces = (center, (col_inner_ref, col_outer_ref), (row_inner_ref, row_outer_ref))
    fill_parts(table_ref, turned_ref, meta_ref, pieces, 0, part_ref, ext_ref, rows_ref, spec_ref)
    flow = flow_ref[...] + placed_flows(
        meta_ref, prior_ref, order_ref, lag_ref, cross_ref, first_ref, part_ref, sec_count - 1, flow_ref.shape, sizes
    )
    for g in range(size_gz):
        for r in range(size_row):
            out_ref[(g * size_row + r) * size_col : (g * size_row + r + 1) * size_col, :] = jnp.broadcast_to(
                flow[r : r + 1, :], (size_col, flow.shape[1])
            )


def exchanges(size):
    inner = [(i, i + 1) for i in range(0, size - 1, 2)]
    outer = [(i, i + 1) for i in range(1, size - 1, 2)]
    return [pairs + [(j, i) for i, j in pairs] for pairs in (inner, outer)]


def match(sections, priors, row_order):
    sec_count, side = sections.shape[:2]
    per_side = side // STRIDE
    place_count = per_side * per_side
    size_gz, size_row, size_col = (lax.axis_size(a) for a in AXES)
    table, lag_table = frequency_tables()
    turned = jnp.asarray(table.T).astype(jnp.bfloat16)
    table = jnp.asarray(table).astype(jnp.bfloat16)
    lag_table = jnp.asarray(np.stack(np.split(lag_table, PATCH // 128, axis=1))).astype(jnp.bfloat16).astype(jnp.float32)
    meta = jnp.stack([lax.axis_index(a) for a in AXES]).astype(jnp.int32)
    wide = side + HALO
    vmem = pl.BlockSpec(memory_space=pltpu.VMEM)
    smem = pl.BlockSpec(memory_space=pltpu.SMEM)
    params = pltpu.CompilerParams(vmem_limit_bytes=VMEM_LIMIT)
    small = pltpu.CompilerParams(vmem_limit_bytes=VMEM_LIMIT // 4)

    def pixels(*shape):
        return jax.ShapeDtypeStruct(shape, jnp.bfloat16)

    gz_pairs = [(i, (i - 1) % size_gz) for i in range(size_gz)]
    col_inner, col_outer = exchanges(size_col)
    row_inner, row_outer = exchanges(size_row)
    glue_cost = pl.CostEstimate(flops=GLUE_FLOPS, bytes_accessed=0, transcendentals=0)
    cuts = pl.pallas_call(
        cut_kernel,
        out_shape=[pixels(sec_count, side, MARGIN)] * 2 + [pixels(sec_count, MARGIN, side)] * 2 + [pixels(1, side, MARGIN)] * 2 + [pixels(1, side, side - HALO), pixels(*sections.shape)],
        in_specs=[smem, vmem],
        out_specs=[vmem] * 8,
        compiler_params=small,
        cost_estimate=glue_cost,
        name="cut",
    )(meta, sections)
    own = cuts[7]
    own_cols = (lax.ppermute(cuts[0], "col", col_inner), lax.ppermute(cuts[1], "col", col_outer))
    own_rows = (lax.ppermute(cuts[2], "row", row_inner), lax.ppermute(cuts[3], "row", row_outer))
    first_inner = lax.ppermute(cuts[4], "gz", gz_pairs)
    first_outer = lax.ppermute(cuts[5], "gz", gz_pairs)
    middle = lax.ppermute(cuts[6], "gz", gz_pairs)
    last_cols = (lax.ppermute(first_inner, "col", col_inner), lax.ppermute(first_outer, "col", col_outer))

    def edges(count, center, cols, width):
        call = pl.pallas_call(
            edge_kernel,
            out_shape=[pixels(count, MARGIN, width)] * 2,
            in_specs=[smem] + [vmem] * (len(center) + 2),
            out_specs=[vmem] * 2,
            compiler_params=small,
            cost_estimate=glue_cost,
        )
        inner, outer = call(meta, *center, *cols)
        return lax.ppermute(inner, "row", row_inner), lax.ppermute(outer, "row", row_outer)

    last_center = (middle, first_inner, first_outer)
    own_corners = edges(sec_count, (), own_cols, HALO)
    last_rows = edges(1, last_center, last_cols, wide)
    lanes = (row_order.shape[0] // size_row) * 2 * size_gz * sec_count * size_col * per_side
    devices = size_gz * size_row * size_col
    sizes = (size_gz, size_row, size_col, sec_count, per_side)
    parts = (place_count, PATCH, PATCH)

    part_shape = jax.ShapeDtypeStruct(parts, jnp.float32)
    flow_shape = jax.ShapeDtypeStruct((size_row, lanes), jnp.float32)
    ext_scratch = pltpu.VMEM((wide, wide), jnp.bfloat16)
    rows_scratch = pltpu.VMEM((per_side, wide, PATCH), jnp.bfloat16)
    spec_scratch = pltpu.VMEM((2, PATCH, PATCH), jnp.float32)
    part_scratch = pltpu.VMEM(parts, jnp.float32)
    cross_scratch = pltpu.VMEM((place_count, PATCH, PATCH), jnp.bfloat16)
    spectra_cost = 2 * per_side * wide * PATCH * PATCH + 2 * place_count * PATCH**3
    pair_cost = 2 * place_count * PATCH * LAGS * (PATCH + LAGS)

    def cost(flops):
        return pl.CostEstimate(flops=flops, bytes_accessed=place_count * PATCH * PATCH * 4, transcendentals=0)

    flow = jnp.zeros((size_row, lanes), jnp.float32)
    pieces = (own, *own_cols, *own_rows, *own_corners)
    first_call = pl.pallas_call(
        functools.partial(first_kernel, section=0),
        out_shape=part_shape,
        in_specs=[smem] + [vmem] * 9,
        out_specs=vmem,
        scratch_shapes=[ext_scratch, rows_scratch, spec_scratch],
        compiler_params=params,
        cost_estimate=cost(spectra_cost),
        name="first",
    )
    part = first_call(meta, table, turned, *pieces)
    for section in range(1, sec_count):
        next_call = pl.pallas_call(
            functools.partial(next_kernel, section=section, sizes=sizes),
            out_shape=(part_shape, flow_shape),
            in_specs=[smem] * 3 + [vmem] * 12,
            out_specs=(vmem, vmem),
            scratch_shapes=[ext_scratch, rows_scratch, spec_scratch, cross_scratch],
            compiler_params=params,
            cost_estimate=cost(spectra_cost + pair_cost),
            name="next",
        )
        part, flow = next_call(meta, priors, row_order, table, turned, *pieces, lag_table, flow, part)
    sent = pl.pallas_call(
        functools.partial(last_kernel, sizes=sizes),
        out_shape=jax.ShapeDtypeStruct((devices, lanes), jnp.float32),
        in_specs=[smem] * 3 + [vmem] * 12,
        out_specs=vmem,
        scratch_shapes=[ext_scratch, rows_scratch, spec_scratch, part_scratch, cross_scratch],
        compiler_params=params,
        cost_estimate=cost(spectra_cost + pair_cost),
        name="last",
    )(meta, priors, row_order, table, turned, lag_table, *last_center, *last_cols, *last_rows, flow, part)
    received = lax.all_to_all(sent, AXES, 0, 0, tiled=True)
    return jnp.sum(received, axis=0).reshape(row_order.shape[0] // size_row, -1)


def solution(mesh):
    placed = (P("gz", "row", "col"), P(None, "gz", "row", "col"), P())
    return jax.shard_map(match, mesh=mesh, in_specs=placed, out_specs=P("row", None), check_vma=False)
```

```python
import functools
import math

import jax
import jax.numpy as jnp
import numpy as np
from jax import lax
from jax.experimental import pallas as pl
from jax.experimental.pallas import tpu as pltpu
from jax.sharding import PartitionSpec as P


PATCH = 512
STRIDE = 256
LAGS = 128
MAXOFF = 64
HALO = 256
HALF = PATCH // 2
MARGIN = HALO // 2
AXES = ("gz", "row", "col")
VMEM_LIMIT = 16 * 1024 * 1024
CHUNK = 16
GLUE_FLOPS = 4 * 10**9


def frequency_tables():
    frequencies = np.concatenate([np.arange(0, HALF, 2), np.arange(1, HALF, 2)])[:, None]
    places = np.arange(PATCH)[None, :]
    step = 2.0 * math.pi / PATCH
    cosine = np.cos(np.mod(frequencies * places, PATCH) * step)
    sine_part = np.sin(np.mod(frequencies * places, PATCH) * step)
    sine_part[0] = np.cos(np.mod(HALF * places[0], PATCH) * step)
    quarter = HALF // 2
    table = np.concatenate([cosine[:quarter], sine_part[:quarter], cosine[quarter:], sine_part[quarter:]], axis=0)
    lags = np.arange(-MAXOFF - LAGS // 2, MAXOFF + LAGS // 2) % PATCH
    return table[:, :HALF].astype(np.float32), table.T[lags].astype(np.float32)


def blocks():
    quarter = HALF // 2
    for k_odd in range(2):
        for l_odd in range(2):
            cols = slice(l_odd * HALF, l_odd * HALF + quarter)
            for start in range(0, quarter, CHUNK):
                yield slice(k_odd * HALF + start, k_odd * HALF + start + CHUNK), cols


def sines(part):
    return slice(part.start + HALF // 2, part.stop + HALF // 2)


def split_parts(spec_ref, out_ref):
    for rows, cols in blocks():
        cc = spec_ref[rows, cols]
        cs = spec_ref[rows, sines(cols)]
        sc = spec_ref[sines(rows), cols]
        ss = spec_ref[sines(rows), sines(cols)]
        a, b, c, d = cc - ss, sc + cs, cc + ss, sc - cs
        if cols.start == 0:
            edge = lax.broadcasted_iota(jnp.int32, cc.shape, 1) == 0
            a, b, c, d = jnp.where(edge, cc, a), jnp.where(edge, sc, b), jnp.where(edge, cs, c), jnp.where(edge, ss, d)
        if rows.start == 0:
            edge = lax.broadcasted_iota(jnp.int32, cc.shape, 0) == 0
            a, b, c, d = jnp.where(edge, cc, a), jnp.where(edge, cs, b), jnp.where(edge, sc, c), jnp.where(edge, ss, d)
        out_ref[rows, cols] = a
        out_ref[rows, sines(cols)] = b
        out_ref[sines(rows), cols] = c
        out_ref[sines(rows), sines(cols)] = d


def cross_parts(first_ref, second_ref, out_ref):
    for rows, cols in blocks():
        places = ((rows, cols), (rows, sines(cols)), (sines(rows), cols), (sines(rows), sines(cols)))
        a, b, c, d = (first_ref[place] for place in places)
        e, f, g, h = (second_ref[place] for place in places)
        p, u = a * e + b * f, a * f - b * e
        q, v = c * g + d * h, c * h - d * g
        cc, cs, sc, ss = p + q, u - v, u + v, q - p
        if cols.start == 0:
            edge = lax.broadcasted_iota(jnp.int32, cc.shape, 1) == 0
            cc, cs, sc, ss = jnp.where(edge, p, cc), jnp.where(edge, q, cs), jnp.where(edge, u, sc), jnp.where(edge, v, ss)
        if rows.start == 0:
            row = lax.broadcasted_iota(jnp.int32, cc.shape, 0) == 0
            cc, cs, sc, ss = jnp.where(row, p, cc), jnp.where(row, u, cs), jnp.where(row, q, sc), jnp.where(row, v, ss)
            if cols.start == 0:
                corner = jnp.logical_and(row, edge)
                cc, cs = jnp.where(corner, 0.5 * (a * e), cc), jnp.where(corner, 0.5 * (b * f), cs)
                sc, ss = jnp.where(corner, 0.5 * (c * g), sc), jnp.where(corner, 0.5 * (d * h), ss)
        for place, value in zip(places, (cc, cs, sc, ss)):
            out_ref[place] = value.astype(jnp.bfloat16)


def lag_rows(lag_ref, offset):
    pieces = [lag_ref[n, pl.ds(offset + MAXOFF, LAGS), :] for n in range(lag_ref.shape[0])]
    return jnp.concatenate(pieces, axis=1).astype(jnp.bfloat16)


def is_even(axis):
    return lax.axis_index(axis) % 2 == 0


def fill_parts(table_ref, turned_ref, pieces, s, out_ref, ext_ref, rows_ref, spec_ref):
    center_refs, col_refs, row_refs = pieces
    top = ext_ref.shape[0] - MARGIN
    row_even, col_even = is_even("row"), is_even("col")
    if len(row_refs) == 2:
        spans = ((row_refs, slice(None), slice(None)),)
    else:
        corners = row_refs[2:]
        spans = (
            (row_refs[:2], slice(None), slice(MARGIN, top)),
            (corners, slice(0, MARGIN), slice(0, MARGIN)),
            (corners, slice(MARGIN, 2 * MARGIN), slice(top, top + MARGIN)),
        )
    for refs, source, target in spans:
        inner, outer = refs[0][s, :, source], refs[1][s, :, source]
        ext_ref[0:MARGIN, target] = lax.select(row_even, outer, inner)
        ext_ref[top:, target] = lax.select(row_even, inner, outer)
    inner, outer = col_refs[0][s], col_refs[1][s]
    ext_ref[MARGIN:top, 0:MARGIN] = lax.select(col_even, outer, inner)
    ext_ref[MARGIN:top, top:] = lax.select(col_even, inner, outer)
    center_rows(ext_ref.at[MARGIN:top, MARGIN:top], col_even, center_refs, s, slice(0, top - MARGIN))
    per_side = (top - MARGIN) // STRIDE
    parities = (slice(0, HALF), slice(HALF, PATCH))
    for pj in range(per_side):
        near = ext_ref[:, pj * STRIDE : pj * STRIDE + HALF]
        away = ext_ref[:, pj * STRIDE + HALF : pj * STRIDE + PATCH]
        for part, folded in zip(parities, (near + away, near - away)):
            rows_ref[pj, :, part] = jnp.dot(folded, turned_ref[:, part], preferred_element_type=jnp.float32).astype(jnp.bfloat16)
        for pi in range(per_side):
            n = pi * per_side + pj
            near = rows_ref[pj, pi * STRIDE : pi * STRIDE + HALF, :]
            away = rows_ref[pj, pi * STRIDE + HALF : pi * STRIDE + PATCH, :]
            for part, folded in zip(parities, (near + away, near - away)):
                spec_ref[n % 2, part] = jnp.dot(table_ref[part], folded, preferred_element_type=jnp.float32)
            split_parts(spec_ref.at[n % 2], out_ref.at[n])


def center_rows(out_ref, col_even, center_refs, s, rows):
    if len(center_refs) == 1:
        out_ref[...] = center_refs[0][s, rows]
        return
    middle_ref, inner_ref, outer_ref = center_refs
    side = out_ref.shape[1]
    inner, outer = inner_ref[s, rows], outer_ref[s, rows]
    out_ref[:, 0:MARGIN] = lax.select(col_even, outer, inner)
    out_ref[:, MARGIN : side - MARGIN] = middle_ref[s, rows]
    out_ref[:, side - MARGIN :] = lax.select(col_even, inner, outer)


def cut_kernel(
    far_ref, inner_ref, outer_ref, row_inner_ref, row_outer_ref, first_inner_ref, first_outer_ref, middle_ref, own_ref,
):
    own_ref[...] = far_ref[...]
    side = own_ref.shape[2]
    row_even, col_even = is_even("row"), is_even("col")
    for s in range(own_ref.shape[0]):
        low, high = own_ref[s, :, 0:MARGIN], own_ref[s, :, side - MARGIN :]
        inner_ref[s] = lax.select(col_even, high, low)
        outer_ref[s] = lax.select(col_even, low, high)
        low, high = own_ref[s, 0:MARGIN, :], own_ref[s, side - MARGIN :, :]
        row_inner_ref[s] = lax.select(row_even, high, low)
        row_outer_ref[s] = lax.select(row_even, low, high)
    low, high = own_ref[0, :, 0:MARGIN], own_ref[0, :, side - MARGIN :]
    first_inner_ref[0] = lax.select(col_even, high, low)
    first_outer_ref[0] = lax.select(col_even, low, high)
    middle_ref[0] = own_ref[0, :, MARGIN : side - MARGIN]


def edge_kernel(*refs):
    *center_refs, col_inner_ref, col_outer_ref, inner_ref, outer_ref = refs
    side, wide = col_inner_ref.shape[1], inner_ref.shape[2]
    row_even, col_even = is_even("row"), is_even("col")
    low, high = slice(0, MARGIN), slice(side - MARGIN, side)
    for s in range(inner_ref.shape[0]):
        for ref, even_rows, odd_rows in ((inner_ref, high, low), (outer_ref, low, high)):
            def pick(source):
                return lax.select(row_even, source[s, even_rows, :], source[s, odd_rows, :])

            inner, outer = pick(col_inner_ref), pick(col_outer_ref)
            ref[s, :, 0:MARGIN] = lax.select(col_even, outer, inner)
            ref[s, :, wide - MARGIN :] = lax.select(col_even, inner, outer)
            if center_refs:
                middle_ref, first_inner_ref, first_outer_ref = center_refs
                inner, outer = pick(first_inner_ref), pick(first_outer_ref)
                ref[s, :, MARGIN : 2 * MARGIN] = lax.select(col_even, outer, inner)
                ref[s, :, 2 * MARGIN : side] = pick(middle_ref)
                ref[s, :, side : side + MARGIN] = lax.select(col_even, inner, outer)


def placed_flows(prior_ref, order_ref, lag_ref, cross_ref, first_ref, second_ref, s, shape, sizes):
    size_gz, size_row, size_col, sec_count, per_side = sizes
    place_count = per_side * per_side
    lanes_each = 2 * size_gz * sec_count * size_col * per_side
    row_count = size_row * per_side
    rows_each = row_count // size_row
    holder = lax.broadcasted_iota(jnp.int32, shape, 0)
    lane = lax.broadcasted_iota(jnp.int32, shape, 1)
    slot = jnp.zeros(shape, jnp.int32)
    for m in range(row_count):
        here = jnp.logical_and(holder == m // rows_each, lane // lanes_each == m % rows_each)
        slot = jnp.where(here, order_ref[m], slot)
    lane = lane % lanes_each
    my_gz, my_row, my_col = (lax.axis_index(a) for a in AXES)
    total_out = jnp.zeros(shape, jnp.float32)
    scale = 2.0 / float(PATCH) ** 3
    down = (lax.broadcasted_iota(jnp.int32, (LAGS, LAGS), 0) - LAGS // 2).astype(jnp.float32)
    across = (lax.broadcasted_iota(jnp.int32, (1, LAGS), 1) - LAGS // 2).astype(jnp.float32)
    sums = []
    for n in range(place_count):
        pi, pj = n // per_side, n % per_side
        cross_parts(first_ref.at[n], second_ref.at[n], cross_ref.at[n])
        row_lags = lag_rows(lag_ref, prior_ref[0, s, pi, pj])
        col_lags = lag_rows(lag_ref, prior_ref[1, s, pi, pj])
        half = jnp.dot(row_lags, cross_ref[n], preferred_element_type=jnp.float32).astype(jnp.bfloat16)
        surface = scale * lax.dot_general(
            half, col_lags, (((1,), (1,)), ((), ())), preferred_element_type=jnp.float32
        )
        weights = surface * surface
        plain = jnp.sum(weights, axis=0, keepdims=True)
        sums += [plain, jnp.sum(weights * down, axis=0, keepdims=True), plain * across]
    sums = jnp.sum(jnp.concatenate(sums, axis=0), axis=1, keepdims=True)
    for n in range(place_count):
        pi, pj = n // per_side, n % per_side
        total = 1.0 + sums[3 * n : 3 * n + 1]
        place = (my_gz * sec_count + s) * (size_col * per_side) + my_col * per_side + pj
        for c in range(2):
            value = prior_ref[c, s, pi, pj].astype(jnp.float32) + sums[3 * n + 1 + c : 3 * n + 2 + c] / total
            here = jnp.logical_and(slot == my_row * per_side + pi, lane == place + c * (lanes_each // 2))
            total_out += jnp.where(here, value, 0.0)
    return total_out


def first_kernel(
    table_ref, turned_ref, own_ref, col_inner_ref, col_outer_ref, row_inner_ref, row_outer_ref,
    corner_inner_ref, corner_outer_ref, part_ref, ext_ref, rows_ref, spec_ref, *, section,
):
    pieces = ((own_ref,), (col_inner_ref, col_outer_ref), (row_inner_ref, row_outer_ref, corner_inner_ref, corner_outer_ref))
    fill_parts(table_ref, turned_ref, pieces, section, part_ref, ext_ref, rows_ref, spec_ref)


def next_kernel(
    far_prior_ref, far_order_ref, table_ref, turned_ref, own_ref, col_inner_ref, col_outer_ref, row_inner_ref, row_outer_ref,
    corner_inner_ref, corner_outer_ref, lag_ref, flow_in_ref, before_ref, part_ref, flow_ref, ext_ref, rows_ref, spec_ref, cross_ref, prior_ref, order_ref, sems,
    *, section, sizes,
):
    pieces = ((own_ref,), (col_inner_ref, col_outer_ref), (row_inner_ref, row_outer_ref, corner_inner_ref, corner_outer_ref))
    copies = (
        pltpu.make_async_copy(far_prior_ref, prior_ref, sems.at[0]),
        pltpu.make_async_copy(far_order_ref, order_ref, sems.at[1]),
    )
    for copy in copies:
        copy.start()
    fill_parts(table_ref, turned_ref, pieces, section, part_ref, ext_ref, rows_ref, spec_ref)
    for copy in copies:
        copy.wait()
    flow_ref[...] = flow_in_ref[...] + placed_flows(
        prior_ref, order_ref, lag_ref, cross_ref, before_ref, part_ref, section - 1, flow_ref.shape, sizes
    )


def last_kernel(
    far_prior_ref, far_order_ref, table_ref, turned_ref, lag_ref, middle_ref, first_inner_ref, first_outer_ref, col_inner_ref, col_outer_ref,
    row_inner_ref, row_outer_ref, flow_ref, first_ref, out_ref, ext_ref, rows_ref, spec_ref, part_ref, cross_ref, prior_ref, order_ref, sems,
    *, sizes,
):
    size_gz, size_row, size_col, sec_count, _ = sizes
    center = (middle_ref, first_inner_ref, first_outer_ref)
    pieces = (center, (col_inner_ref, col_outer_ref), (row_inner_ref, row_outer_ref))
    copies = (
        pltpu.make_async_copy(far_prior_ref, prior_ref, sems.at[0]),
        pltpu.make_async_copy(far_order_ref, order_ref, sems.at[1]),
    )
    for copy in copies:
        copy.start()
    fill_parts(table_ref, turned_ref, pieces, 0, part_ref, ext_ref, rows_ref, spec_ref)
    for copy in copies:
        copy.wait()
    flow = flow_ref[...] + placed_flows(
        prior_ref, order_ref, lag_ref, cross_ref, first_ref, part_ref, sec_count - 1, flow_ref.shape, sizes
    )
    for g in range(size_gz):
        for r in range(size_row):
            out_ref[(g * size_row + r) * size_col : (g * size_row + r + 1) * size_col, :] = jnp.broadcast_to(
                flow[r : r + 1, :], (size_col, flow.shape[1])
            )


def exchanges(size):
    inner = [(i, i + 1) for i in range(0, size - 1, 2)]
    outer = [(i, i + 1) for i in range(1, size - 1, 2)]
    return [pairs + [(j, i) for i, j in pairs] for pairs in (inner, outer)]


def match(sections, priors, row_order):
    sec_count, side = sections.shape[:2]
    per_side = side // STRIDE
    place_count = per_side * per_side
    size_gz, size_row, size_col = (lax.axis_size(a) for a in AXES)
    table, lag_table = frequency_tables()
    turned = jnp.asarray(table.T).astype(jnp.bfloat16)
    table = jnp.asarray(table).astype(jnp.bfloat16)
    lag_table = jnp.asarray(np.stack(np.split(lag_table, PATCH // 128, axis=1))).astype(jnp.bfloat16).astype(jnp.float32)
    wide = side + HALO
    vmem = pl.BlockSpec(memory_space=pltpu.VMEM)
    far = pl.BlockSpec(memory_space=pl.ANY)
    params = pltpu.CompilerParams(vmem_limit_bytes=VMEM_LIMIT)
    small = pltpu.CompilerParams(vmem_limit_bytes=VMEM_LIMIT // 4)

    def pixels(*shape):
        return jax.ShapeDtypeStruct(shape, jnp.bfloat16)

    gz_pairs = [(i, (i - 1) % size_gz) for i in range(size_gz)]
    col_inner, col_outer = exchanges(size_col)
    row_inner, row_outer = exchanges(size_row)
    glue_cost = pl.CostEstimate(flops=GLUE_FLOPS, bytes_accessed=0, transcendentals=0)
    cuts = pl.pallas_call(
        cut_kernel,
        out_shape=[pixels(sec_count, side, MARGIN)] * 2 + [pixels(sec_count, MARGIN, side)] * 2 + [pixels(1, side, MARGIN)] * 2 + [pixels(1, side, side - HALO), pixels(*sections.shape)],
        in_specs=[vmem],
        out_specs=[vmem] * 8,
        compiler_params=small,
        cost_estimate=glue_cost,
        name="cut",
    )(sections)
    own = cuts[7]
    own_cols = (lax.ppermute(cuts[0], "col", col_inner), lax.ppermute(cuts[1], "col", col_outer))
    own_rows = (lax.ppermute(cuts[2], "row", row_inner), lax.ppermute(cuts[3], "row", row_outer))
    first_inner = lax.ppermute(cuts[4], "gz", gz_pairs)
    first_outer = lax.ppermute(cuts[5], "gz", gz_pairs)
    middle = lax.ppermute(cuts[6], "gz", gz_pairs)
    last_cols = (lax.ppermute(first_inner, "col", col_inner), lax.ppermute(first_outer, "col", col_outer))

    def edges(count, center, cols, width):
        call = pl.pallas_call(
            edge_kernel,
            out_shape=[pixels(count, MARGIN, width)] * 2,
            in_specs=[vmem] * (len(center) + 2),
            out_specs=[vmem] * 2,
            compiler_params=small,
            cost_estimate=glue_cost,
        )
        inner, outer = call(*center, *cols)
        return lax.ppermute(inner, "row", row_inner), lax.ppermute(outer, "row", row_outer)

    last_center = (middle, first_inner, first_outer)
    own_corners = edges(sec_count, (), own_cols, HALO)
    last_rows = edges(1, last_center, last_cols, wide)
    lanes = (row_order.shape[0] // size_row) * 2 * size_gz * sec_count * size_col * per_side
    devices = size_gz * size_row * size_col
    sizes = (size_gz, size_row, size_col, sec_count, per_side)
    parts = (place_count, PATCH, PATCH)

    part_shape = jax.ShapeDtypeStruct(parts, jnp.float32)
    flow_shape = jax.ShapeDtypeStruct((size_row, lanes), jnp.float32)
    ext_scratch = pltpu.VMEM((wide, wide), jnp.bfloat16)
    rows_scratch = pltpu.VMEM((per_side, wide, PATCH), jnp.bfloat16)
    spec_scratch = pltpu.VMEM((2, PATCH, PATCH), jnp.float32)
    part_scratch = pltpu.VMEM(parts, jnp.float32)
    scalars = [
        pltpu.SMEM(priors.shape, priors.dtype),
        pltpu.SMEM(row_order.shape, row_order.dtype),
        pltpu.SemaphoreType.DMA((2,)),
    ]
    cross_scratch = pltpu.VMEM((place_count, PATCH, PATCH), jnp.bfloat16)
    spectra_cost = 2 * per_side * wide * PATCH * PATCH + 2 * place_count * PATCH**3
    pair_cost = 2 * place_count * PATCH * LAGS * (PATCH + LAGS)

    def cost(flops):
        return pl.CostEstimate(flops=flops, bytes_accessed=place_count * PATCH * PATCH * 4, transcendentals=0)

    flow = jnp.zeros((size_row, lanes), jnp.float32)
    pieces = (own, *own_cols, *own_rows, *own_corners)
    first_call = pl.pallas_call(
        functools.partial(first_kernel, section=0),
        out_shape=part_shape,
        in_specs=[vmem] * 9,
        out_specs=vmem,
        scratch_shapes=[ext_scratch, rows_scratch, spec_scratch],
        compiler_params=params,
        cost_estimate=cost(spectra_cost),
        name="first",
    )
    part = first_call(table, turned, *pieces)
    for section in range(1, sec_count):
        next_call = pl.pallas_call(
            functools.partial(next_kernel, section=section, sizes=sizes),
            out_shape=(part_shape, flow_shape),
            in_specs=[far] * 2 + [vmem] * 12,
            out_specs=(vmem, vmem),
            scratch_shapes=[ext_scratch, rows_scratch, spec_scratch, cross_scratch, *scalars],
            compiler_params=params,
            cost_estimate=cost(spectra_cost + pair_cost),
            name="next",
        )
        part, flow = next_call(priors, row_order, table, turned, *pieces, lag_table, flow, part)
    sent = pl.pallas_call(
        functools.partial(last_kernel, sizes=sizes),
        out_shape=jax.ShapeDtypeStruct((devices, lanes), jnp.float32),
        in_specs=[far] * 2 + [vmem] * 12,
        out_specs=vmem,
        scratch_shapes=[ext_scratch, rows_scratch, spec_scratch, part_scratch, cross_scratch, *scalars],
        compiler_params=params,
        cost_estimate=cost(spectra_cost + pair_cost),
        name="last",
    )(priors, row_order, table, turned, lag_table, *last_center, *last_cols, *last_rows, flow, part)
    received = lax.all_to_all(sent, AXES, 0, 0, tiled=True)
    return jnp.sum(received, axis=0).reshape(row_order.shape[0] // size_row, -1)


def solution(mesh):
    placed = (P("gz", "row", "col"), P(None, "gz", "row", "col"), P())
    return jax.shard_map(match, mesh=mesh, in_specs=placed, out_specs=P("row", None), check_vma=False)
```

```python
import functools
import math

import jax
import jax.numpy as jnp
import numpy as np
from jax import lax
from jax.experimental import pallas as pl
from jax.experimental.pallas import tpu as pltpu
from jax.sharding import PartitionSpec as P


PATCH = 512
STRIDE = 256
LAGS = 128
MAXOFF = 64
HALO = 256
HALF = PATCH // 2
MARGIN = HALO // 2
AXES = ("gz", "row", "col")
VMEM_LIMIT = 16 * 1024 * 1024
CHUNK = 16
GLUE_FLOPS = 4 * 10**9


def frequency_tables():
    frequencies = np.concatenate([np.arange(0, HALF, 2), np.arange(1, HALF, 2)])[:, None]
    places = np.arange(PATCH)[None, :]
    step = 2.0 * math.pi / PATCH
    cosine = np.cos(np.mod(frequencies * places, PATCH) * step)
    sine_part = np.sin(np.mod(frequencies * places, PATCH) * step)
    sine_part[0] = np.cos(np.mod(HALF * places[0], PATCH) * step)
    quarter = HALF // 2
    table = np.concatenate([cosine[:quarter], sine_part[:quarter], cosine[quarter:], sine_part[quarter:]], axis=0)
    lags = np.arange(-MAXOFF - LAGS // 2, MAXOFF + LAGS // 2) % PATCH
    return table[:, :HALF].astype(np.float32), table.T[lags].astype(np.float32)


def blocks():
    quarter = HALF // 2
    for k_odd in range(2):
        for l_odd in range(2):
            cols = slice(l_odd * HALF, l_odd * HALF + quarter)
            for start in range(0, quarter, CHUNK):
                yield slice(k_odd * HALF + start, k_odd * HALF + start + CHUNK), cols


def sines(part):
    return slice(part.start + HALF // 2, part.stop + HALF // 2)


def split_parts(spec_ref, out_ref):
    for rows, cols in blocks():
        cc = spec_ref[rows, cols]
        cs = spec_ref[rows, sines(cols)]
        sc = spec_ref[sines(rows), cols]
        ss = spec_ref[sines(rows), sines(cols)]
        a, b, c, d = cc - ss, sc + cs, cc + ss, sc - cs
        if cols.start == 0:
            edge = lax.broadcasted_iota(jnp.int32, cc.shape, 1) == 0
            a, b, c, d = jnp.where(edge, cc, a), jnp.where(edge, sc, b), jnp.where(edge, cs, c), jnp.where(edge, ss, d)
        if rows.start == 0:
            edge = lax.broadcasted_iota(jnp.int32, cc.shape, 0) == 0
            a, b, c, d = jnp.where(edge, cc, a), jnp.where(edge, cs, b), jnp.where(edge, sc, c), jnp.where(edge, ss, d)
        out_ref[rows, cols] = a
        out_ref[rows, sines(cols)] = b
        out_ref[sines(rows), cols] = c
        out_ref[sines(rows), sines(cols)] = d


def cross_parts(first_ref, second_ref, out_ref):
    for rows, cols in blocks():
        places = ((rows, cols), (rows, sines(cols)), (sines(rows), cols), (sines(rows), sines(cols)))
        a, b, c, d = (first_ref[place] for place in places)
        e, f, g, h = (second_ref[place] for place in places)
        p, u = a * e + b * f, a * f - b * e
        q, v = c * g + d * h, c * h - d * g
        cc, cs, sc, ss = p + q, u - v, u + v, q - p
        if cols.start == 0:
            edge = lax.broadcasted_iota(jnp.int32, cc.shape, 1) == 0
            cc, cs, sc, ss = jnp.where(edge, p, cc), jnp.where(edge, q, cs), jnp.where(edge, u, sc), jnp.where(edge, v, ss)
        if rows.start == 0:
            row = lax.broadcasted_iota(jnp.int32, cc.shape, 0) == 0
            cc, cs, sc, ss = jnp.where(row, p, cc), jnp.where(row, u, cs), jnp.where(row, q, sc), jnp.where(row, v, ss)
            if cols.start == 0:
                corner = jnp.logical_and(row, edge)
                cc, cs = jnp.where(corner, 0.5 * (a * e), cc), jnp.where(corner, 0.5 * (b * f), cs)
                sc, ss = jnp.where(corner, 0.5 * (c * g), sc), jnp.where(corner, 0.5 * (d * h), ss)
        for place, value in zip(places, (cc, cs, sc, ss)):
            out_ref[place] = value.astype(jnp.bfloat16)


def lag_rows(lag_ref, offset):
    pieces = [lag_ref[n, pl.ds(offset + MAXOFF, LAGS), :] for n in range(lag_ref.shape[0])]
    return jnp.concatenate(pieces, axis=1).astype(jnp.bfloat16)


def is_even(axis):
    return lax.axis_index(axis) % 2 == 0


def fill_center(ext_ref, center_refs, col_refs, s):
    top = ext_ref.shape[1] - MARGIN
    col_even = is_even("col")
    inner, outer = col_refs[0][s], col_refs[1][s]
    ext_ref[:, 0:MARGIN] = lax.select(col_even, outer, inner)
    ext_ref[:, top:] = lax.select(col_even, inner, outer)
    center_rows(ext_ref.at[:, MARGIN:top], col_even, center_refs, s, slice(0, top - MARGIN))


def fill_edge(ext_ref, row_refs, s):
    top = ext_ref.shape[1] - MARGIN
    row_even = is_even("row")
    if len(row_refs) == 2:
        spans = ((row_refs, slice(None), slice(None)),)
    else:
        corners = row_refs[2:]
        spans = (
            (row_refs[:2], slice(None), slice(MARGIN, top)),
            (corners, slice(0, MARGIN), slice(0, MARGIN)),
            (corners, slice(MARGIN, 2 * MARGIN), slice(top, top + MARGIN)),
        )
    for refs, source, target in spans:
        inner, outer = refs[0][s, :, source], refs[1][s, :, source]
        ext_ref[0:MARGIN, target] = lax.select(row_even, outer, inner)
        ext_ref[MARGIN:, target] = lax.select(row_even, inner, outer)


PARITIES = (slice(0, HALF), slice(HALF, PATCH))


def row_pass(ext_ref, turned_ref, out_ref):
    for pj in range(out_ref.shape[0]):
        near = ext_ref[:, pj * STRIDE : pj * STRIDE + HALF]
        away = ext_ref[:, pj * STRIDE + HALF : pj * STRIDE + PATCH]
        for part, folded in zip(PARITIES, (near + away, near - away)):
            found = jnp.dot(folded, turned_ref[:, part], preferred_element_type=jnp.float32)
            out_ref[pj, :, part] = found.astype(jnp.bfloat16)


def column_pass(table_ref, middle_ref, edge_ref, spec_ref, out_ref):
    per_side, side = middle_ref.shape[:2]
    bounds = (0, MARGIN, side + MARGIN, side + HALO)

    def rows(pj, start, stop):
        found = []
        for ref, shift, low, high in (
            (edge_ref, 0, bounds[0], bounds[1]),
            (middle_ref, MARGIN, bounds[1], bounds[2]),
            (edge_ref, side, bounds[2], bounds[3]),
        ):
            low, high = max(low, start), min(high, stop)
            if low < high:
                found.append(ref[pj, low - shift : high - shift, :])
        return found[0] if len(found) == 1 else jnp.concatenate(found, axis=0)

    for pj in range(per_side):
        for pi in range(per_side):
            n = pi * per_side + pj
            near = rows(pj, pi * STRIDE, pi * STRIDE + HALF)
            away = rows(pj, pi * STRIDE + HALF, pi * STRIDE + PATCH)
            for part, folded in zip(PARITIES, (near + away, near - away)):
                spec_ref[n % 2, part] = jnp.dot(table_ref[part], folded, preferred_element_type=jnp.float32)
            split_parts(spec_ref.at[n % 2], out_ref.at[n])


def center_rows(out_ref, col_even, center_refs, s, rows):
    if len(center_refs) == 1:
        out_ref[...] = center_refs[0][s, rows]
        return
    middle_ref, inner_ref, outer_ref = center_refs
    side = out_ref.shape[1]
    inner, outer = inner_ref[s, rows], outer_ref[s, rows]
    out_ref[:, 0:MARGIN] = lax.select(col_even, outer, inner)
    out_ref[:, MARGIN : side - MARGIN] = middle_ref[s, rows]
    out_ref[:, side - MARGIN :] = lax.select(col_even, inner, outer)


def cut_kernel(
    far_ref, inner_ref, outer_ref, row_inner_ref, row_outer_ref, first_inner_ref, first_outer_ref, middle_ref, own_ref,
):
    own_ref[...] = far_ref[...]
    side = own_ref.shape[2]
    row_even, col_even = is_even("row"), is_even("col")
    for s in range(own_ref.shape[0]):
        low, high = own_ref[s, :, 0:MARGIN], own_ref[s, :, side - MARGIN :]
        inner_ref[s] = lax.select(col_even, high, low)
        outer_ref[s] = lax.select(col_even, low, high)
        low, high = own_ref[s, 0:MARGIN, :], own_ref[s, side - MARGIN :, :]
        row_inner_ref[s] = lax.select(row_even, high, low)
        row_outer_ref[s] = lax.select(row_even, low, high)
    low, high = own_ref[0, :, 0:MARGIN], own_ref[0, :, side - MARGIN :]
    first_inner_ref[0] = lax.select(col_even, high, low)
    first_outer_ref[0] = lax.select(col_even, low, high)
    middle_ref[0] = own_ref[0, :, MARGIN : side - MARGIN]


def edge_kernel(*refs):
    *center_refs, col_inner_ref, col_outer_ref, inner_ref, outer_ref = refs
    side, wide = col_inner_ref.shape[1], inner_ref.shape[2]
    row_even, col_even = is_even("row"), is_even("col")
    low, high = slice(0, MARGIN), slice(side - MARGIN, side)
    for s in range(inner_ref.shape[0]):
        for ref, even_rows, odd_rows in ((inner_ref, high, low), (outer_ref, low, high)):
            def pick(source):
                return lax.select(row_even, source[s, even_rows, :], source[s, odd_rows, :])

            inner, outer = pick(col_inner_ref), pick(col_outer_ref)
            ref[s, :, 0:MARGIN] = lax.select(col_even, outer, inner)
            ref[s, :, wide - MARGIN :] = lax.select(col_even, inner, outer)
            if center_refs:
                middle_ref, first_inner_ref, first_outer_ref = center_refs
                inner, outer = pick(first_inner_ref), pick(first_outer_ref)
                ref[s, :, MARGIN : 2 * MARGIN] = lax.select(col_even, outer, inner)
                ref[s, :, 2 * MARGIN : side] = pick(middle_ref)
                ref[s, :, side : side + MARGIN] = lax.select(col_even, inner, outer)


def placed_flows(prior_ref, order_ref, lag_ref, cross_ref, first_ref, second_ref, s, shape, sizes):
    size_gz, size_row, size_col, sec_count, per_side = sizes
    place_count = per_side * per_side
    lanes_each = 2 * size_gz * sec_count * size_col * per_side
    row_count = size_row * per_side
    rows_each = row_count // size_row
    holder = lax.broadcasted_iota(jnp.int32, shape, 0)
    lane = lax.broadcasted_iota(jnp.int32, shape, 1)
    slot = jnp.zeros(shape, jnp.int32)
    for m in range(row_count):
        here = jnp.logical_and(holder == m // rows_each, lane // lanes_each == m % rows_each)
        slot = jnp.where(here, order_ref[m], slot)
    lane = lane % lanes_each
    my_gz, my_row, my_col = (lax.axis_index(a) for a in AXES)
    total_out = jnp.zeros(shape, jnp.float32)
    scale = 2.0 / float(PATCH) ** 3
    down = (lax.broadcasted_iota(jnp.int32, (LAGS, LAGS), 0) - LAGS // 2).astype(jnp.float32)
    across = (lax.broadcasted_iota(jnp.int32, (1, LAGS), 1) - LAGS // 2).astype(jnp.float32)
    sums = []
    for n in range(place_count):
        pi, pj = n // per_side, n % per_side
        cross_parts(first_ref.at[n], second_ref.at[n], cross_ref.at[n])
        row_lags = lag_rows(lag_ref, prior_ref[0, s, pi, pj])
        col_lags = lag_rows(lag_ref, prior_ref[1, s, pi, pj])
        half = jnp.dot(row_lags, cross_ref[n], preferred_element_type=jnp.float32).astype(jnp.bfloat16)
        surface = scale * lax.dot_general(
            half, col_lags, (((1,), (1,)), ((), ())), preferred_element_type=jnp.float32
        )
        weights = surface * surface
        plain = jnp.sum(weights, axis=0, keepdims=True)
        sums += [plain, jnp.sum(weights * down, axis=0, keepdims=True), plain * across]
    sums = jnp.sum(jnp.concatenate(sums, axis=0), axis=1, keepdims=True)
    for n in range(place_count):
        pi, pj = n // per_side, n % per_side
        total = 1.0 + sums[3 * n : 3 * n + 1]
        place = (my_gz * sec_count + s) * (size_col * per_side) + my_col * per_side + pj
        for c in range(2):
            value = prior_ref[c, s, pi, pj].astype(jnp.float32) + sums[3 * n + 1 + c : 3 * n + 2 + c] / total
            here = jnp.logical_and(slot == my_row * per_side + pi, lane == place + c * (lanes_each // 2))
            total_out += jnp.where(here, value, 0.0)
    return total_out


def rows_kernel(turned_ref, own_ref, col_inner_ref, col_outer_ref, rows_ref, ext_ref):
    for s in range(own_ref.shape[0]):
        fill_center(ext_ref.at[s], (own_ref,), (col_inner_ref, col_outer_ref), s)
        row_pass(ext_ref.at[s], turned_ref, rows_ref.at[s])


def last_rows_kernel(
    turned_ref, middle_ref, first_inner_ref, first_outer_ref, col_inner_ref, col_outer_ref, rows_ref, ext_ref,
):
    fill_center(ext_ref, (middle_ref, first_inner_ref, first_outer_ref), (col_inner_ref, col_outer_ref), 0)
    row_pass(ext_ref, turned_ref, rows_ref)


def own_parts(table_ref, turned_ref, middle_ref, row_refs, section, part_ref, ext_ref, rows_ref, spec_ref):
    fill_edge(ext_ref, row_refs, section)
    row_pass(ext_ref, turned_ref, rows_ref)
    column_pass(table_ref, middle_ref.at[section], rows_ref, spec_ref, part_ref)


def first_kernel(
    table_ref, turned_ref, middle_ref, row_inner_ref, row_outer_ref, corner_inner_ref, corner_outer_ref,
    part_ref, ext_ref, rows_ref, spec_ref, *, section,
):
    row_refs = (row_inner_ref, row_outer_ref, corner_inner_ref, corner_outer_ref)
    own_parts(table_ref, turned_ref, middle_ref, row_refs, section, part_ref, ext_ref, rows_ref, spec_ref)


def next_kernel(
    far_prior_ref, far_order_ref, table_ref, turned_ref, middle_ref, row_inner_ref, row_outer_ref,
    corner_inner_ref, corner_outer_ref, lag_ref, flow_in_ref, before_ref, part_ref, flow_ref,
    ext_ref, rows_ref, spec_ref, cross_ref, prior_ref, order_ref, sems, *, section, sizes,
):
    row_refs = (row_inner_ref, row_outer_ref, corner_inner_ref, corner_outer_ref)
    copies = (
        pltpu.make_async_copy(far_prior_ref, prior_ref, sems.at[0]),
        pltpu.make_async_copy(far_order_ref, order_ref, sems.at[1]),
    )
    for copy in copies:
        copy.start()
    own_parts(table_ref, turned_ref, middle_ref, row_refs, section, part_ref, ext_ref, rows_ref, spec_ref)
    for copy in copies:
        copy.wait()
    flow_ref[...] = flow_in_ref[...] + placed_flows(
        prior_ref, order_ref, lag_ref, cross_ref, before_ref, part_ref, section - 1, flow_ref.shape, sizes
    )


def last_kernel(
    far_prior_ref, far_order_ref, table_ref, turned_ref, lag_ref, middle_ref, row_inner_ref, row_outer_ref,
    flow_ref, first_ref, out_ref, ext_ref, rows_ref, spec_ref, part_ref, cross_ref, prior_ref, order_ref, sems, *, sizes,
):
    size_gz, size_row, size_col, sec_count, _ = sizes
    copies = (
        pltpu.make_async_copy(far_prior_ref, prior_ref, sems.at[0]),
        pltpu.make_async_copy(far_order_ref, order_ref, sems.at[1]),
    )
    for copy in copies:
        copy.start()
    fill_edge(ext_ref, (row_inner_ref, row_outer_ref), 0)
    row_pass(ext_ref, turned_ref, rows_ref)
    column_pass(table_ref, middle_ref, rows_ref, spec_ref, part_ref)
    for copy in copies:
        copy.wait()
    flow = flow_ref[...] + placed_flows(
        prior_ref, order_ref, lag_ref, cross_ref, first_ref, part_ref, sec_count - 1, flow_ref.shape, sizes
    )
    for g in range(size_gz):
        for r in range(size_row):
            out_ref[(g * size_row + r) * size_col : (g * size_row + r + 1) * size_col, :] = jnp.broadcast_to(
                flow[r : r + 1, :], (size_col, flow.shape[1])
            )


def exchanges(size):
    inner = [(i, i + 1) for i in range(0, size - 1, 2)]
    outer = [(i, i + 1) for i in range(1, size - 1, 2)]
    return [pairs + [(j, i) for i, j in pairs] for pairs in (inner, outer)]


def match(sections, priors, row_order):
    sec_count, side = sections.shape[:2]
    per_side = side // STRIDE
    place_count = per_side * per_side
    size_gz, size_row, size_col = (lax.axis_size(a) for a in AXES)
    table, lag_table = frequency_tables()
    turned = jnp.asarray(table.T).astype(jnp.bfloat16)
    table = jnp.asarray(table).astype(jnp.bfloat16)
    lag_table = jnp.asarray(np.stack(np.split(lag_table, PATCH // 128, axis=1))).astype(jnp.bfloat16).astype(jnp.float32)
    wide = side + HALO
    vmem = pl.BlockSpec(memory_space=pltpu.VMEM)
    far = pl.BlockSpec(memory_space=pl.ANY)
    params = pltpu.CompilerParams(vmem_limit_bytes=VMEM_LIMIT)
    small = pltpu.CompilerParams(vmem_limit_bytes=VMEM_LIMIT // 4)

    def pixels(*shape):
        return jax.ShapeDtypeStruct(shape, jnp.bfloat16)

    gz_pairs = [(i, (i - 1) % size_gz) for i in range(size_gz)]
    col_inner, col_outer = exchanges(size_col)
    row_inner, row_outer = exchanges(size_row)
    glue_cost = pl.CostEstimate(flops=GLUE_FLOPS, bytes_accessed=0, transcendentals=0)
    cuts = pl.pallas_call(
        cut_kernel,
        out_shape=[pixels(sec_count, side, MARGIN)] * 2 + [pixels(sec_count, MARGIN, side)] * 2 + [pixels(1, side, MARGIN)] * 2 + [pixels(1, side, side - HALO), pixels(*sections.shape)],
        in_specs=[vmem],
        out_specs=[vmem] * 8,
        compiler_params=small,
        cost_estimate=glue_cost,
        name="cut",
    )(sections)
    own = cuts[7]
    own_cols = (lax.ppermute(cuts[0], "col", col_inner), lax.ppermute(cuts[1], "col", col_outer))
    own_rows = (lax.ppermute(cuts[2], "row", row_inner), lax.ppermute(cuts[3], "row", row_outer))
    first_inner = lax.ppermute(cuts[4], "gz", gz_pairs)
    first_outer = lax.ppermute(cuts[5], "gz", gz_pairs)
    middle = lax.ppermute(cuts[6], "gz", gz_pairs)
    last_cols = (lax.ppermute(first_inner, "col", col_inner), lax.ppermute(first_outer, "col", col_outer))

    def edges(count, center, cols, width):
        call = pl.pallas_call(
            edge_kernel,
            out_shape=[pixels(count, MARGIN, width)] * 2,
            in_specs=[vmem] * (len(center) + 2),
            out_specs=[vmem] * 2,
            compiler_params=small,
            cost_estimate=glue_cost,
        )
        inner, outer = call(*center, *cols)
        return lax.ppermute(inner, "row", row_inner), lax.ppermute(outer, "row", row_outer)

    last_center = (middle, first_inner, first_outer)
    own_corners = edges(sec_count, (), own_cols, HALO)
    last_rows = edges(1, last_center, last_cols, wide)
    lanes = (row_order.shape[0] // size_row) * 2 * size_gz * sec_count * size_col * per_side
    devices = size_gz * size_row * size_col
    sizes = (size_gz, size_row, size_col, sec_count, per_side)
    parts = (place_count, PATCH, PATCH)

    part_shape = jax.ShapeDtypeStruct(parts, jnp.float32)
    flow_shape = jax.ShapeDtypeStruct((size_row, lanes), jnp.float32)
    edge_ext_scratch = pltpu.VMEM((HALO, wide), jnp.bfloat16)
    edge_rows_scratch = pltpu.VMEM((per_side, HALO, PATCH), jnp.bfloat16)
    spec_scratch = pltpu.VMEM((2, PATCH, PATCH), jnp.float32)
    part_scratch = pltpu.VMEM(parts, jnp.float32)
    scalars = [
        pltpu.SMEM(priors.shape, priors.dtype),
        pltpu.SMEM(row_order.shape, row_order.dtype),
        pltpu.SemaphoreType.DMA((2,)),
    ]
    cross_scratch = pltpu.VMEM((place_count, PATCH, PATCH), jnp.bfloat16)
    spectra_cost = 2 * per_side * wide * PATCH * PATCH + 2 * place_count * PATCH**3
    pair_cost = 2 * place_count * PATCH * LAGS * (PATCH + LAGS)

    def cost(flops):
        return pl.CostEstimate(flops=flops, bytes_accessed=place_count * PATCH * PATCH * 4, transcendentals=0)

    flow = jnp.zeros((size_row, lanes), jnp.float32)
    rows_call = pl.pallas_call(
        rows_kernel,
        out_shape=pixels(sec_count, per_side, side, PATCH),
        in_specs=[vmem] * 4,
        out_specs=vmem,
        scratch_shapes=[pltpu.VMEM((sec_count, side, wide), jnp.bfloat16)],
        compiler_params=params,
        cost_estimate=cost(2 * sec_count * per_side * side * HALF * PATCH),
        name="rows",
    )
    own_middle = rows_call(turned, own, *own_cols)
    pieces = (own_middle, *own_rows, *own_corners)
    first_call = pl.pallas_call(
        functools.partial(first_kernel, section=0),
        out_shape=part_shape,
        in_specs=[vmem] * 7,
        out_specs=vmem,
        scratch_shapes=[edge_ext_scratch, edge_rows_scratch, spec_scratch],
        compiler_params=params,
        cost_estimate=cost(spectra_cost),
        name="first",
    )
    part = first_call(table, turned, *pieces)
    for section in range(1, sec_count):
        next_call = pl.pallas_call(
            functools.partial(next_kernel, section=section, sizes=sizes),
            out_shape=(part_shape, flow_shape),
            in_specs=[far] * 2 + [vmem] * 10,
            out_specs=(vmem, vmem),
            scratch_shapes=[edge_ext_scratch, edge_rows_scratch, spec_scratch, cross_scratch, *scalars],
            compiler_params=params,
            cost_estimate=cost(spectra_cost + pair_cost),
            name="next",
        )
        part, flow = next_call(priors, row_order, table, turned, *pieces, lag_table, flow, part)
    last_rows_call = pl.pallas_call(
        last_rows_kernel,
        out_shape=pixels(per_side, side, PATCH),
        in_specs=[vmem] * 6,
        out_specs=vmem,
        scratch_shapes=[pltpu.VMEM((side, wide), jnp.bfloat16)],
        compiler_params=params,
        cost_estimate=cost(2 * per_side * side * HALF * PATCH),
        name="last_middle",
    )
    last_middle = last_rows_call(turned, *last_center, *last_cols)
    sent = pl.pallas_call(
        functools.partial(last_kernel, sizes=sizes),
        out_shape=jax.ShapeDtypeStruct((devices, lanes), jnp.float32),
        in_specs=[far] * 2 + [vmem] * 8,
        out_specs=vmem,
        scratch_shapes=[edge_ext_scratch, edge_rows_scratch, spec_scratch, part_scratch, cross_scratch, *scalars],
        compiler_params=params,
        cost_estimate=cost(spectra_cost + pair_cost),
        name="last",
    )(priors, row_order, table, turned, lag_table, last_middle, *last_rows, flow, part)
    received = lax.all_to_all(sent, AXES, 0, 0, tiled=True)
    return jnp.sum(received, axis=0).reshape(row_order.shape[0] // size_row, -1)


def solution(mesh):
    placed = (P("gz", "row", "col"), P(None, "gz", "row", "col"), P())
    return jax.shard_map(match, mesh=mesh, in_specs=placed, out_specs=P("row", None), check_vma=False)
```

```python
import functools
import math

import jax
import jax.numpy as jnp
import numpy as np
from jax import lax
from jax.experimental import pallas as pl
from jax.experimental.pallas import tpu as pltpu
from jax.sharding import PartitionSpec as P


PATCH = 512
STRIDE = 256
LAGS = 128
MAXOFF = 64
HALO = 256
HALF = PATCH // 2
MARGIN = HALO // 2
AXES = ("gz", "row", "col")
VMEM_LIMIT = 16 * 1024 * 1024
CHUNK = 16
GLUE_FLOPS = 4 * 10**9


def frequency_tables():
    frequencies = np.concatenate([np.arange(0, HALF, 2), np.arange(1, HALF, 2)])[:, None]
    places = np.arange(PATCH)[None, :]
    step = 2.0 * math.pi / PATCH
    cosine = np.cos(np.mod(frequencies * places, PATCH) * step)
    sine_part = np.sin(np.mod(frequencies * places, PATCH) * step)
    sine_part[0] = np.cos(np.mod(HALF * places[0], PATCH) * step)
    quarter = HALF // 2
    table = np.concatenate([cosine[:quarter], sine_part[:quarter], cosine[quarter:], sine_part[quarter:]], axis=0)
    lags = np.arange(-MAXOFF - LAGS // 2, MAXOFF + LAGS // 2) % PATCH
    return table[:, :HALF].astype(np.float32), table.T[lags].astype(np.float32)


def blocks():
    quarter = HALF // 2
    for k_odd in range(2):
        for l_odd in range(2):
            cols = slice(l_odd * HALF, l_odd * HALF + quarter)
            for start in range(0, quarter, CHUNK):
                yield slice(k_odd * HALF + start, k_odd * HALF + start + CHUNK), cols


def sines(part):
    return slice(part.start + HALF // 2, part.stop + HALF // 2)


def split_parts(spec_ref, out_ref):
    for rows, cols in blocks():
        cc = spec_ref[rows, cols]
        cs = spec_ref[rows, sines(cols)]
        sc = spec_ref[sines(rows), cols]
        ss = spec_ref[sines(rows), sines(cols)]
        a, b, c, d = cc - ss, sc + cs, cc + ss, sc - cs
        if cols.start == 0:
            edge = lax.broadcasted_iota(jnp.int32, cc.shape, 1) == 0
            a, b, c, d = jnp.where(edge, cc, a), jnp.where(edge, sc, b), jnp.where(edge, cs, c), jnp.where(edge, ss, d)
        if rows.start == 0:
            edge = lax.broadcasted_iota(jnp.int32, cc.shape, 0) == 0
            a, b, c, d = jnp.where(edge, cc, a), jnp.where(edge, cs, b), jnp.where(edge, sc, c), jnp.where(edge, ss, d)
        out_ref[rows, cols] = a
        out_ref[rows, sines(cols)] = b
        out_ref[sines(rows), cols] = c
        out_ref[sines(rows), sines(cols)] = d


def cross_parts(first_ref, second_ref, out_ref):
    for rows, cols in blocks():
        places = ((rows, cols), (rows, sines(cols)), (sines(rows), cols), (sines(rows), sines(cols)))
        a, b, c, d = (first_ref[place] for place in places)
        e, f, g, h = (second_ref[place] for place in places)
        p, u = a * e + b * f, a * f - b * e
        q, v = c * g + d * h, c * h - d * g
        cc, cs, sc, ss = p + q, u - v, u + v, q - p
        if cols.start == 0:
            edge = lax.broadcasted_iota(jnp.int32, cc.shape, 1) == 0
            cc, cs, sc, ss = jnp.where(edge, p, cc), jnp.where(edge, q, cs), jnp.where(edge, u, sc), jnp.where(edge, v, ss)
        if rows.start == 0:
            row = lax.broadcasted_iota(jnp.int32, cc.shape, 0) == 0
            cc, cs, sc, ss = jnp.where(row, p, cc), jnp.where(row, u, cs), jnp.where(row, q, sc), jnp.where(row, v, ss)
            if cols.start == 0:
                corner = jnp.logical_and(row, edge)
                cc, cs = jnp.where(corner, 0.5 * (a * e), cc), jnp.where(corner, 0.5 * (b * f), cs)
                sc, ss = jnp.where(corner, 0.5 * (c * g), sc), jnp.where(corner, 0.5 * (d * h), ss)
        for place, value in zip(places, (cc, cs, sc, ss)):
            out_ref[place] = value.astype(jnp.bfloat16)


def lag_rows(lag_ref, offset):
    pieces = [lag_ref[n, pl.ds(offset + MAXOFF, LAGS), :] for n in range(lag_ref.shape[0])]
    return jnp.concatenate(pieces, axis=1).astype(jnp.bfloat16)


def is_even(axis):
    return lax.axis_index(axis) % 2 == 0


def fill_center(ext_ref, center_refs, col_refs, s):
    top = ext_ref.shape[1] - MARGIN
    col_even = is_even("col")
    inner, outer = col_refs[0][s], col_refs[1][s]
    ext_ref[:, 0:MARGIN] = lax.select(col_even, outer, inner)
    ext_ref[:, top:] = lax.select(col_even, inner, outer)
    center_rows(ext_ref.at[:, MARGIN:top], col_even, center_refs, s, slice(0, top - MARGIN))


def fill_edge(ext_ref, row_refs, s):
    top = ext_ref.shape[1] - MARGIN
    row_even = is_even("row")
    if len(row_refs) == 2:
        spans = ((row_refs, slice(None), slice(None)),)
    else:
        corners = row_refs[2:]
        spans = (
            (row_refs[:2], slice(None), slice(MARGIN, top)),
            (corners, slice(0, MARGIN), slice(0, MARGIN)),
            (corners, slice(MARGIN, 2 * MARGIN), slice(top, top + MARGIN)),
        )
    for refs, source, target in spans:
        inner, outer = refs[0][s, :, source], refs[1][s, :, source]
        ext_ref[0:MARGIN, target] = lax.select(row_even, outer, inner)
        ext_ref[MARGIN:, target] = lax.select(row_even, inner, outer)


PARITIES = (slice(0, HALF), slice(HALF, PATCH))


def row_pass(ext_ref, turned_ref, out_ref):
    for pj in range(out_ref.shape[0]):
        near = ext_ref[:, pj * STRIDE : pj * STRIDE + HALF]
        away = ext_ref[:, pj * STRIDE + HALF : pj * STRIDE + PATCH]
        for part, folded in zip(PARITIES, (near + away, near - away)):
            found = jnp.dot(folded, turned_ref[:, part], preferred_element_type=jnp.float32)
            out_ref[pj, :, part] = found.astype(jnp.bfloat16)


def column_pass(table_ref, middle_ref, edge_ref, spec_ref, out_ref):
    per_side, side = middle_ref.shape[:2]
    bounds = (0, MARGIN, side + MARGIN, side + HALO)

    def rows(pj, start, stop):
        found = []
        for ref, shift, low, high in (
            (edge_ref, 0, bounds[0], bounds[1]),
            (middle_ref, MARGIN, bounds[1], bounds[2]),
            (edge_ref, side, bounds[2], bounds[3]),
        ):
            low, high = max(low, start), min(high, stop)
            if low < high:
                found.append(ref[pj, low - shift : high - shift, :])
        return found[0] if len(found) == 1 else jnp.concatenate(found, axis=0)

    for pj in range(per_side):
        for pi in range(per_side):
            n = pi * per_side + pj
            near = rows(pj, pi * STRIDE, pi * STRIDE + HALF)
            away = rows(pj, pi * STRIDE + HALF, pi * STRIDE + PATCH)
            for part, folded in zip(PARITIES, (near + away, near - away)):
                spec_ref[n % 2, part] = jnp.dot(table_ref[part], folded, preferred_element_type=jnp.float32)
            split_parts(spec_ref.at[n % 2], out_ref.at[n])


def center_rows(out_ref, col_even, center_refs, s, rows):
    if len(center_refs) == 1:
        out_ref[...] = center_refs[0][s, rows]
        return
    middle_ref, inner_ref, outer_ref = center_refs
    side = out_ref.shape[1]
    inner, outer = inner_ref[s, rows], outer_ref[s, rows]
    out_ref[:, 0:MARGIN] = lax.select(col_even, outer, inner)
    out_ref[:, MARGIN : side - MARGIN] = middle_ref[s, rows]
    out_ref[:, side - MARGIN :] = lax.select(col_even, inner, outer)


def cut_kernel(
    far_ref, inner_ref, outer_ref, row_inner_ref, row_outer_ref, first_inner_ref, first_outer_ref, middle_ref, own_ref,
):
    own_ref[...] = far_ref[...]
    side = own_ref.shape[2]
    row_even, col_even = is_even("row"), is_even("col")
    for s in range(own_ref.shape[0]):
        low, high = own_ref[s, :, 0:MARGIN], own_ref[s, :, side - MARGIN :]
        inner_ref[s] = lax.select(col_even, high, low)
        outer_ref[s] = lax.select(col_even, low, high)
        low, high = own_ref[s, 0:MARGIN, :], own_ref[s, side - MARGIN :, :]
        row_inner_ref[s] = lax.select(row_even, high, low)
        row_outer_ref[s] = lax.select(row_even, low, high)
    low, high = own_ref[0, :, 0:MARGIN], own_ref[0, :, side - MARGIN :]
    first_inner_ref[0] = lax.select(col_even, high, low)
    first_outer_ref[0] = lax.select(col_even, low, high)
    middle_ref[0] = own_ref[0, :, MARGIN : side - MARGIN]


def edge_kernel(*refs):
    *center_refs, col_inner_ref, col_outer_ref, inner_ref, outer_ref = refs
    side, wide = col_inner_ref.shape[1], inner_ref.shape[2]
    row_even, col_even = is_even("row"), is_even("col")
    low, high = slice(0, MARGIN), slice(side - MARGIN, side)
    for s in range(inner_ref.shape[0]):
        for ref, even_rows, odd_rows in ((inner_ref, high, low), (outer_ref, low, high)):
            def pick(source):
                return lax.select(row_even, source[s, even_rows, :], source[s, odd_rows, :])

            inner, outer = pick(col_inner_ref), pick(col_outer_ref)
            ref[s, :, 0:MARGIN] = lax.select(col_even, outer, inner)
            ref[s, :, wide - MARGIN :] = lax.select(col_even, inner, outer)
            if center_refs:
                middle_ref, first_inner_ref, first_outer_ref = center_refs
                inner, outer = pick(first_inner_ref), pick(first_outer_ref)
                ref[s, :, MARGIN : 2 * MARGIN] = lax.select(col_even, outer, inner)
                ref[s, :, 2 * MARGIN : side] = pick(middle_ref)
                ref[s, :, side : side + MARGIN] = lax.select(col_even, inner, outer)


def placed_flows(prior_ref, order_ref, lag_ref, cross_ref, first_ref, second_ref, s, shape, sizes):
    size_gz, size_row, size_col, sec_count, per_side = sizes
    place_count = per_side * per_side
    lanes_each = 2 * size_gz * sec_count * size_col * per_side
    row_count = size_row * per_side
    rows_each = row_count // size_row
    holder = lax.broadcasted_iota(jnp.int32, shape, 0)
    lane = lax.broadcasted_iota(jnp.int32, shape, 1)
    slot = jnp.zeros(shape, jnp.int32)
    for m in range(row_count):
        here = jnp.logical_and(holder == m // rows_each, lane // lanes_each == m % rows_each)
        slot = jnp.where(here, order_ref[m], slot)
    lane = lane % lanes_each
    my_gz, my_row, my_col = (lax.axis_index(a) for a in AXES)
    total_out = jnp.zeros(shape, jnp.float32)
    scale = 2.0 / float(PATCH) ** 3
    down = (lax.broadcasted_iota(jnp.int32, (LAGS, LAGS), 0) - LAGS // 2).astype(jnp.float32)
    across = (lax.broadcasted_iota(jnp.int32, (1, LAGS), 1) - LAGS // 2).astype(jnp.float32)
    sums = []
    for n in range(place_count):
        pi, pj = n // per_side, n % per_side
        cross_parts(first_ref.at[n], second_ref.at[n], cross_ref.at[n])
        row_lags = lag_rows(lag_ref, prior_ref[0, s, pi, pj])
        col_lags = lag_rows(lag_ref, prior_ref[1, s, pi, pj])
        half = jnp.dot(row_lags, cross_ref[n], preferred_element_type=jnp.float32).astype(jnp.bfloat16)
        surface = scale * lax.dot_general(
            half, col_lags, (((1,), (1,)), ((), ())), preferred_element_type=jnp.float32
        )
        weights = surface * surface
        plain = jnp.sum(weights, axis=0, keepdims=True)
        sums += [plain, jnp.sum(weights * down, axis=0, keepdims=True), plain * across]
    sums = jnp.sum(jnp.concatenate(sums, axis=0), axis=1, keepdims=True)
    for n in range(place_count):
        pi, pj = n // per_side, n % per_side
        total = 1.0 + sums[3 * n : 3 * n + 1]
        place = (my_gz * sec_count + s) * (size_col * per_side) + my_col * per_side + pj
        for c in range(2):
            value = prior_ref[c, s, pi, pj].astype(jnp.float32) + sums[3 * n + 1 + c : 3 * n + 2 + c] / total
            here = jnp.logical_and(slot == my_row * per_side + pi, lane == place + c * (lanes_each // 2))
            total_out += jnp.where(here, value, 0.0)
    return total_out


def rows_kernel(turned_ref, own_ref, col_inner_ref, col_outer_ref, rows_ref, ext_ref):
    for s in range(own_ref.shape[0]):
        fill_center(ext_ref.at[s], (own_ref,), (col_inner_ref, col_outer_ref), s)
        row_pass(ext_ref.at[s], turned_ref, rows_ref.at[s])


def last_rows_kernel(
    turned_ref, middle_ref, first_inner_ref, first_outer_ref, col_inner_ref, col_outer_ref, rows_ref, ext_ref,
):
    fill_center(ext_ref, (middle_ref, first_inner_ref, first_outer_ref), (col_inner_ref, col_outer_ref), 0)
    row_pass(ext_ref, turned_ref, rows_ref)


def own_parts(table_ref, turned_ref, middle_ref, row_refs, section, part_ref, ext_ref, rows_ref, spec_ref):
    fill_edge(ext_ref, row_refs, section)
    row_pass(ext_ref, turned_ref, rows_ref)
    column_pass(table_ref, middle_ref.at[section], rows_ref, spec_ref, part_ref)


def own_kernel(
    far_prior_ref, far_order_ref, table_ref, turned_ref, middle_ref, row_inner_ref, row_outer_ref,
    corner_inner_ref, corner_outer_ref, lag_ref, part_ref, flow_ref,
    ext_ref, rows_ref, spec_ref, before_ref, cross_ref, prior_ref, order_ref, sems, *, sizes,
):
    row_refs = (row_inner_ref, row_outer_ref, corner_inner_ref, corner_outer_ref)
    copies = (
        pltpu.make_async_copy(far_prior_ref, prior_ref, sems.at[0]),
        pltpu.make_async_copy(far_order_ref, order_ref, sems.at[1]),
    )
    for copy in copies:
        copy.start()
    sec_count = middle_ref.shape[0]
    flow = jnp.zeros(flow_ref.shape, jnp.float32)
    for section in range(sec_count):
        here = part_ref if section == sec_count - 1 else before_ref.at[section]
        own_parts(
            table_ref, turned_ref, middle_ref, row_refs, section, here, ext_ref.at[section], rows_ref.at[section], spec_ref,
        )
        if section == min(1, sec_count - 1):
            for copy in copies:
                copy.wait()
        if section > 0:
            flow += placed_flows(
                prior_ref, order_ref, lag_ref, cross_ref, before_ref.at[section - 1], here, section - 1, flow.shape, sizes
            )
    flow_ref[...] = flow


def last_kernel(
    far_prior_ref, far_order_ref, table_ref, turned_ref, lag_ref, middle_ref, row_inner_ref, row_outer_ref,
    flow_ref, first_ref, out_ref, ext_ref, rows_ref, spec_ref, part_ref, cross_ref, prior_ref, order_ref, sems, *, sizes,
):
    size_gz, size_row, size_col, sec_count, _ = sizes
    copies = (
        pltpu.make_async_copy(far_prior_ref, prior_ref, sems.at[0]),
        pltpu.make_async_copy(far_order_ref, order_ref, sems.at[1]),
    )
    for copy in copies:
        copy.start()
    fill_edge(ext_ref, (row_inner_ref, row_outer_ref), 0)
    row_pass(ext_ref, turned_ref, rows_ref)
    column_pass(table_ref, middle_ref, rows_ref, spec_ref, part_ref)
    for copy in copies:
        copy.wait()
    flow = flow_ref[...] + placed_flows(
        prior_ref, order_ref, lag_ref, cross_ref, first_ref, part_ref, sec_count - 1, flow_ref.shape, sizes
    )
    for g in range(size_gz):
        for r in range(size_row):
            out_ref[(g * size_row + r) * size_col : (g * size_row + r + 1) * size_col, :] = jnp.broadcast_to(
                flow[r : r + 1, :], (size_col, flow.shape[1])
            )


def exchanges(size):
    inner = [(i, i + 1) for i in range(0, size - 1, 2)]
    outer = [(i, i + 1) for i in range(1, size - 1, 2)]
    return [pairs + [(j, i) for i, j in pairs] for pairs in (inner, outer)]


def match(sections, priors, row_order):
    sec_count, side = sections.shape[:2]
    per_side = side // STRIDE
    place_count = per_side * per_side
    size_gz, size_row, size_col = (lax.axis_size(a) for a in AXES)
    table, lag_table = frequency_tables()
    turned = jnp.asarray(table.T).astype(jnp.bfloat16)
    table = jnp.asarray(table).astype(jnp.bfloat16)
    lag_table = jnp.asarray(np.stack(np.split(lag_table, PATCH // 128, axis=1))).astype(jnp.bfloat16).astype(jnp.float32)
    wide = side + HALO
    vmem = pl.BlockSpec(memory_space=pltpu.VMEM)
    far = pl.BlockSpec(memory_space=pl.ANY)
    params = pltpu.CompilerParams(vmem_limit_bytes=VMEM_LIMIT)
    small = pltpu.CompilerParams(vmem_limit_bytes=VMEM_LIMIT // 4)

    def pixels(*shape):
        return jax.ShapeDtypeStruct(shape, jnp.bfloat16)

    gz_pairs = [(i, (i - 1) % size_gz) for i in range(size_gz)]
    col_inner, col_outer = exchanges(size_col)
    row_inner, row_outer = exchanges(size_row)
    glue_cost = pl.CostEstimate(flops=GLUE_FLOPS, bytes_accessed=0, transcendentals=0)
    cuts = pl.pallas_call(
        cut_kernel,
        out_shape=[pixels(sec_count, side, MARGIN)] * 2 + [pixels(sec_count, MARGIN, side)] * 2 + [pixels(1, side, MARGIN)] * 2 + [pixels(1, side, side - HALO), pixels(*sections.shape)],
        in_specs=[vmem],
        out_specs=[vmem] * 8,
        compiler_params=small,
        cost_estimate=glue_cost,
        name="cut",
    )(sections)
    own = cuts[7]
    own_cols = (lax.ppermute(cuts[0], "col", col_inner), lax.ppermute(cuts[1], "col", col_outer))
    own_rows = (lax.ppermute(cuts[2], "row", row_inner), lax.ppermute(cuts[3], "row", row_outer))
    first_inner = lax.ppermute(cuts[4], "gz", gz_pairs)
    first_outer = lax.ppermute(cuts[5], "gz", gz_pairs)
    middle = lax.ppermute(cuts[6], "gz", gz_pairs)
    last_cols = (lax.ppermute(first_inner, "col", col_inner), lax.ppermute(first_outer, "col", col_outer))

    def edges(count, center, cols, width):
        call = pl.pallas_call(
            edge_kernel,
            out_shape=[pixels(count, MARGIN, width)] * 2,
            in_specs=[vmem] * (len(center) + 2),
            out_specs=[vmem] * 2,
            compiler_params=small,
            cost_estimate=glue_cost,
        )
        inner, outer = call(*center, *cols)
        return lax.ppermute(inner, "row", row_inner), lax.ppermute(outer, "row", row_outer)

    last_center = (middle, first_inner, first_outer)
    own_corners = edges(sec_count, (), own_cols, HALO)
    last_rows = edges(1, last_center, last_cols, wide)
    lanes = (row_order.shape[0] // size_row) * 2 * size_gz * sec_count * size_col * per_side
    devices = size_gz * size_row * size_col
    sizes = (size_gz, size_row, size_col, sec_count, per_side)
    parts = (place_count, PATCH, PATCH)

    part_shape = jax.ShapeDtypeStruct(parts, jnp.float32)
    flow_shape = jax.ShapeDtypeStruct((size_row, lanes), jnp.float32)
    edge_ext_scratch = pltpu.VMEM((HALO, wide), jnp.bfloat16)
    edge_rows_scratch = pltpu.VMEM((per_side, HALO, PATCH), jnp.bfloat16)
    spec_scratch = pltpu.VMEM((2, PATCH, PATCH), jnp.float32)
    part_scratch = pltpu.VMEM(parts, jnp.float32)
    scalars = [
        pltpu.SMEM(priors.shape, priors.dtype),
        pltpu.SMEM(row_order.shape, row_order.dtype),
        pltpu.SemaphoreType.DMA((2,)),
    ]
    cross_scratch = pltpu.VMEM((place_count, PATCH, PATCH), jnp.bfloat16)
    spectra_cost = 2 * per_side * wide * PATCH * PATCH + 2 * place_count * PATCH**3
    pair_cost = 2 * place_count * PATCH * LAGS * (PATCH + LAGS)

    def cost(flops):
        return pl.CostEstimate(flops=flops, bytes_accessed=place_count * PATCH * PATCH * 4, transcendentals=0)

    rows_call = pl.pallas_call(
        rows_kernel,
        out_shape=pixels(sec_count, per_side, side, PATCH),
        in_specs=[vmem] * 4,
        out_specs=vmem,
        scratch_shapes=[pltpu.VMEM((sec_count, side, wide), jnp.bfloat16)],
        compiler_params=params,
        cost_estimate=cost(2 * sec_count * per_side * side * HALF * PATCH),
        name="rows",
    )
    own_middle = rows_call(turned, own, *own_cols)
    pieces = (own_middle, *own_rows, *own_corners)
    own_call = pl.pallas_call(
        functools.partial(own_kernel, sizes=sizes),
        out_shape=(part_shape, flow_shape),
        in_specs=[far] * 2 + [vmem] * 8,
        out_specs=(vmem, vmem),
        scratch_shapes=[
            pltpu.VMEM((sec_count, HALO, wide), jnp.bfloat16),
            pltpu.VMEM((sec_count, per_side, HALO, PATCH), jnp.bfloat16),
            spec_scratch,
            pltpu.VMEM((max(1, sec_count - 1),) + parts, jnp.float32),
            cross_scratch,
            *scalars,
        ],
        compiler_params=params,
        cost_estimate=cost(sec_count * (spectra_cost + pair_cost)),
        name="own",
    )
    part, flow = own_call(priors, row_order, table, turned, *pieces, lag_table)
    last_rows_call = pl.pallas_call(
        last_rows_kernel,
        out_shape=pixels(per_side, side, PATCH),
        in_specs=[vmem] * 6,
        out_specs=vmem,
        scratch_shapes=[pltpu.VMEM((side, wide), jnp.bfloat16)],
        compiler_params=params,
        cost_estimate=cost(2 * per_side * side * HALF * PATCH),
        name="last_middle",
    )
    last_middle = last_rows_call(turned, *last_center, *last_cols)
    sent = pl.pallas_call(
        functools.partial(last_kernel, sizes=sizes),
        out_shape=jax.ShapeDtypeStruct((devices, lanes), jnp.float32),
        in_specs=[far] * 2 + [vmem] * 8,
        out_specs=vmem,
        scratch_shapes=[edge_ext_scratch, edge_rows_scratch, spec_scratch, part_scratch, cross_scratch, *scalars],
        compiler_params=params,
        cost_estimate=cost(spectra_cost + pair_cost),
        name="last",
    )(priors, row_order, table, turned, lag_table, last_middle, *last_rows, flow, part)
    received = lax.all_to_all(sent, AXES, 0, 0, tiled=True)
    return jnp.sum(received, axis=0).reshape(row_order.shape[0] // size_row, -1)


def solution(mesh):
    placed = (P("gz", "row", "col"), P(None, "gz", "row", "col"), P())
    return jax.shard_map(match, mesh=mesh, in_specs=placed, out_specs=P("row", None), check_vma=False)
```
